32 devices in a mesh: groups: 2 (over y), owners: 4 (over x, core), sub: 4 (over z).
Axes of the slice: x: 2, y: 2, z: 4, core: 2. Of those that a mesh axis runs over, the one named last changes fastest.
Arguments:
- embeddings: bfloat16 [16384, 768], P(('groups', 'owners', 'sub')), parts along dimension 0, may hold values from -6 to 6, as said below
- class_table: bfloat16 [1000, 768], replicated, may hold values from -6 to 6
- nearest: int32 [16384], P(('groups', 'owners', 'sub')), parts along dimension 0, may hold values from 0 to 999
- keep_class: int32 [1000], replicated, may hold values 0 or 1
- destination: int32 [16384, 1], P(('groups', 'owners', 'sub')), parts along dimension 0, may hold values from 0 to 15; in each aligned block of 512 rows (0 to 511, 512 to 1023, ...) at most 48 rows name the same one
Outputs:
- received_rows: bfloat16 [24576, 768], P(('groups', 'owners', 'sub')), parts along dimension 0
- received_score: bfloat16 [24576], P(('groups', 'owners', 'sub')), parts along dimension 0
- received_position: int32 [24576], P(('groups', 'owners', 'sub')), parts along dimension 0
- shard_totals: int32 [32], P('groups'), parts along dimension 0
The draws below stay inside these ranges and needn't reach their ends.
There are 2 independent parts, one for each index of `groups`. The reference program is written for one: setup_inputs(seed, part) draws one part's arguments, and reference() takes and returns one part's arrays. A program takes and returns all parts, laid end to end along the dimension named above; an argument that names none is the same for every part. Nothing has to cross between parts.
Inputs may be any that keep to these rules, and one draw needn't show every extreme that they name: `destination`: in the rows of one device no loader shard is named by more than 48 rows. Counts of rows per loader shard may be packed several to an int32 word wherever they travel; this is an exception to the 4-bit rule below. `embeddings`: some rows are entirely zero.
All inputs are finite; a program needn't handle non-finite values.
Results may differ from the reference program's by a relative error of at most 0.001.
Values may be sent and summed in bfloat16 or wider, within the bound.
A program may use at most 64 MiB of HBM per device.

```python
import math
import jax
import jax.numpy as jnp
import numpy as np
from jax import lax

D = 768
CLASSES = 1000
ROWS_DEV = 512
NDEST = 16
CAP = 48
ROWS = 8192


def draw_embeddings(key, part):
    value_key = jax.random.fold_in(key, 11)
    blank_key = jax.random.fold_in(key, 13)
    values = jnp.clip(jax.random.normal(value_key, (ROWS, D), jnp.float32), -6.0, 6.0)
    blank = jax.random.randint(blank_key, (ROWS, 1), 0, 64) == 0
    values = jnp.where(blank, jnp.float32(0.0), values)
    return values.astype(jnp.bfloat16)


def plant(values, own_key, least, high):
    dims = values.shape
    spot = [jax.random.randint(jax.random.fold_in(own_key, axis), (), 0, dims[axis]) for axis in range(len(dims))]
    values = values.at[tuple(spot)].set(least)
    longest = dims.index(max(dims))
    spot[longest] = (spot[longest] + 1) % dims[longest]
    return values.at[tuple(spot)].set(high)


def routed_block(rng, own, number, rows, count, top, bound, slope):
    ranking = jax.random.permutation(rng, count)
    heavy_load, ordinary = shares(count, rows * top, bound, slope, True), shares(count, rows * top, bound, slope, False)
    places = jnp.arange(count)

    def named(tallies, turn):
        used = int((tallies > 0).sum())
        fixed = max(1, used // 4)
        passed = fixed + (places - fixed + turn * (used - fixed)) % max(1, count - fixed)
        return jnp.zeros((count,), jnp.int32).at[ranking[jnp.where(places < fixed, places, passed)]].set(jnp.asarray(tallies, jnp.int32))

    tallies = jnp.where(number % 4 == 0, named(heavy_load, number // 4), named(ordinary, number - number // 4 - 1))
    mixed = jax.random.permutation(jax.random.fold_in(own, 3), count)
    donor, taker = mixed[0:count // 2 * 2:2], mixed[1:count // 2 * 2:2]
    slack = jnp.minimum(tallies[donor] - 1, bound - tallies[taker]) // 2
    slack = jnp.where((donor == ranking[0]) | (taker == ranking[0]) | (tallies[taker] == 0), 0, jnp.maximum(slack, 0))
    passed = jax.random.randint(jax.random.fold_in(own, 4), (count // 2,), 0, 1 << 20) % (slack + 1)
    tallies = tallies.at[donor].add(-passed).at[taker].add(passed)
    items = jnp.searchsorted(jnp.cumsum(tallies), jnp.arange(rows * top), side="right").astype(jnp.int32)
    table = items.reshape(top, rows).T
    table = table[jax.random.permutation(jax.random.fold_in(own, 1), rows)]
    turn = jax.random.randint(jax.random.fold_in(own, 2), (rows, 1), 0, top)
    return jnp.take_along_axis(table, (jnp.arange(top)[None, :] + turn) % top, axis=1)


def shares(amount, total, bound, lean, full):
    portions = [(1 << 20) // math.isqrt(rank ** lean) + 1 for rank in range(1, amount + 1)]
    largest = bound if full else min(bound, max(-(-total // amount), total * portions[0] // sum(portions)))
    least = 1 if total - largest >= amount - 1 else 0
    holding, rest = [largest] + [least] * (amount - 1), total - largest - least * (amount - 1)
    while rest > 0:
        candidates = [i for i in range(1, amount) if holding[i] < largest] or [i for i in range(1, amount) if holding[i] < bound]
        mass, budget = sum([portions[i] for i in candidates]), rest
        for i in candidates:
            more = min(bound - holding[i], max(1, budget * portions[i] // mass), rest)
            holding[i] = holding[i] + more
            rest = rest - more
    return np.array(holding)


def noise(stream_key, extent, scale, most, kind=jnp.bfloat16):
    return jnp.clip(scale * jax.random.normal(stream_key, extent, jnp.float32), -most, most).astype(kind)


def setup_inputs(seed: int = 0, part: int = 0) -> dict:
    keys = jax.random.split(jax.random.key(seed), 6)
    own_keys = jax.random.split(jax.random.fold_in(keys[5], part), 6)
    embeddings = draw_embeddings(jax.random.fold_in(jax.random.fold_in(keys[5], part), 71), part)
    class_table = noise(keys[1], (CLASSES, D), 1.0, 6.0)
    nearest = plant(jax.random.randint(own_keys[2], (ROWS,), 0, CLASSES), jax.random.fold_in(own_keys[2], 1), 0, CLASSES - 1).astype(jnp.int32)
    keep_class = plant((jax.random.randint(keys[3], (CLASSES,), 0, 4) < 3).astype(jnp.int32), jax.random.fold_in(keys[3], 1), 0, 1)
    destination_keys = jax.random.split(jax.random.fold_in(own_keys[4], 1), ROWS // ROWS_DEV)
    destination_turns = jax.random.permutation(jax.random.fold_in(own_keys[4], 3), ROWS // ROWS_DEV)
    destination = jax.vmap(lambda own, number: routed_block(jax.random.fold_in(own_keys[4], 2), own, number, ROWS_DEV, NDEST, 1, CAP, 2))(destination_keys, destination_turns).reshape((ROWS, 1))
    return dict(embeddings=embeddings, class_table=class_table, nearest=nearest, keep_class=keep_class, destination=destination)


def margins(row_block, near_block, class_table, inverse_class, keep_class):
    products = jnp.dot(row_block, class_table.T, preferred_element_type=jnp.float32)
    squares = row_block.astype(jnp.float32) * row_block.astype(jnp.float32)
    inverse_row = lax.rsqrt(lax.optimization_barrier(jnp.sum(squares, axis=1)) + 1e-06)
    cosine = products * inverse_row[:, None] * inverse_class[None, :]
    class_ids = jnp.arange(class_table.shape[0], dtype=jnp.int32)
    class_match = near_block[:, None] == class_ids[None, :]
    given_cos = lax.optimization_barrier(jnp.sum(jnp.where(class_match, cosine, 0.0), axis=1))
    others = lax.optimization_barrier(jnp.max(jnp.where(class_match, -1e+30, cosine), axis=1))
    kept_flag = lax.optimization_barrier(jnp.sum(jnp.where(class_match, keep_class[None, :], 0), axis=1)).astype(jnp.int32)
    return (20.0 * (given_cos - others), kept_flag)

def reference(embeddings, class_table, nearest, keep_class, destination):
    class_float = class_table.astype(jnp.float32)
    inverse_class = lax.rsqrt(lax.optimization_barrier(jnp.sum(class_float * class_float, axis=1)) + 1e-06)
    total_rows = embeddings.shape[0]
    block_rows = math.gcd(total_rows, 1024)

    def one_block(inputs):
        return margins(inputs[0], inputs[1], class_table, inverse_class, keep_class)
    margin_value, kept_flag = lax.map(one_block, (embeddings.reshape(total_rows // block_rows, block_rows, D), nearest.reshape(total_rows // block_rows, block_rows)))
    margin_value = margin_value.reshape(total_rows)
    kept_flag = kept_flag.reshape(total_rows)
    target = destination[:, 0].astype(jnp.int32)
    shard_ids = jnp.arange(NDEST, dtype=jnp.int32)
    onehot = ((target[:, None] == shard_ids[None, :]) & (kept_flag[:, None] == 1)).astype(jnp.int32)
    running = jnp.cumsum(onehot, axis=0) - onehot
    global_rank = jnp.take_along_axis(running, target[:, None], axis=1)[:, 0].astype(jnp.int32)
    block_start = running.reshape(NDEST, ROWS_DEV, NDEST)[:, 0, :]
    source = (jnp.arange(total_rows, dtype=jnp.int32) // ROWS_DEV).astype(jnp.int32)
    local_rank = (global_rank - block_start[source, target]).astype(jnp.int32)
    slot_count = NDEST * NDEST * CAP
    slot_index = jnp.where(kept_flag == 1, (target * NDEST + source) * CAP + local_rank, slot_count).astype(jnp.int32)
    received_rows = jnp.zeros((slot_count, D), jnp.bfloat16).at[slot_index].set(embeddings, mode='drop')
    received_score = jnp.zeros((slot_count,), jnp.bfloat16).at[slot_index].set(margin_value.astype(jnp.bfloat16), mode='drop')
    received_position = jnp.full((slot_count,), -1, jnp.int32).at[slot_index].set(global_rank, mode='drop')
    shard_totals = lax.optimization_barrier(jnp.sum(onehot, axis=0)).astype(jnp.int32)
    return (received_rows, received_score, received_position, shard_totals)
```

```python
import functools

import jax
import jax.numpy as jnp
from jax import lax
from jax.experimental import pallas as pl
from jax.experimental.pallas import tpu as pltpu
from jax.sharding import PartitionSpec as P

MESH = pl.DeviceIdType.MESH
CROSS = (((1,), (1,)), ((), ()))
DOWN = (((0,), (0,)), ((), ()))


def up(value, step):
    return (value + step - 1) // step * step


def place(owners, subs, k):
    o, z = lax.axis_index("owners"), lax.axis_index("sub")
    upper = (2 * z) // subs
    toward = upper * z + (1 - upper) * (subs - 1 - z)
    j = k // owners
    first = 1 - (j + subs - 1) // subs
    past = (j + subs - toward) // subs
    far = first * toward + (1 - first) * (j + past)
    to_sub = (z + far * (1 - 2 * upper) + subs) % subs
    to_owner = (o + 1 + k % owners) % owners
    return to_owner, to_sub


def finish_kernel(rows_ref, score_ref, position_ref, totals_ref, rows_out, score_out, position_out, totals_out,
                  score_s, position_s, totals_s, sem):
    copies = [pltpu.make_async_copy(rows_ref, rows_out, sem.at[0])]
    copies[0].start()
    position_s[...] = position_ref[...].reshape(position_s.shape)
    totals_s[...] = totals_ref[...].reshape(totals_s.shape)
    score_s[...] = score_ref[...].reshape(score_s.shape).astype(score_s.dtype)
    for i, (inner, outer) in enumerate(((position_s, position_out), (totals_s, totals_out), (score_s, score_out))):
        copies.append(pltpu.make_async_copy(inner, outer, sem.at[i + 1]))
        copies[-1].start()
    for copy in copies:
        copy.wait()


def kernel(owners, subs, cap, early, near_hbm, keep_hbm, dest_hbm, emb_hbm, table_hbm,
           rows_ref, score_ref, position_ref, totals_ref,
           near_ref, keep_ref, dest_ref, emb, table, keep2, send, meta, got, spots, counts_s, scores_s, slot_s,
           in_sem, send_sem, recv_sem, meta_send, meta_recv, own_sem):
    f32, bf16, i32 = jnp.float32, jnp.bfloat16, jnp.int32
    shards = owners * subs
    rows, width = emb.shape
    classes = table.shape[0]
    wide = meta.shape[2]
    slots = shards * cap
    o, z = lax.axis_index("owners"), lax.axis_index("sub")
    own = o * subs + z

    small = [
        pltpu.make_async_copy(near_hbm, near_ref, in_sem.at[2]),
        pltpu.make_async_copy(keep_hbm, keep_ref, in_sem.at[3]),
        pltpu.make_async_copy(dest_hbm, dest_ref, in_sem.at[4]),
    ]
    for copy in small:
        copy.start()
    emb_copy = pltpu.make_async_copy(emb_hbm, emb, in_sem.at[0])
    emb_copy.start()
    table_copy = pltpu.make_async_copy(table_hbm, table, in_sem.at[1])
    table_copy.start()

    barrier = pltpu.get_barrier_semaphore()

    def greet(k, c):
        a, b = place(owners, subs, k)
        pl.semaphore_signal(barrier, inc=1, device_id={"owners": a, "sub": b}, device_id_type=MESH)
        return c

    lax.fori_loop(0, shards - 1, greet, 0)

    for copy in small:
        copy.wait()
    near = near_ref[...]
    target = dest_ref[...]
    keep2[...] = jnp.zeros_like(keep2)
    for h in range(up(classes, 128) // 128):
        n = min(128, classes - h * 128)
        keep2[h : h + 1, :n] = keep_ref[:, h * 128 : h * 128 + n].astype(f32)
    deep = keep2.shape[0]
    high = near // 128
    low = near - high * 128
    low_hot = (lax.broadcasted_iota(i32, (128, rows), 0) == low).astype(f32).astype(bf16)
    by_high = jnp.dot(keep2[...].astype(bf16), low_hot, preferred_element_type=f32)
    kept = jnp.sum(
        jnp.where(lax.broadcasted_iota(i32, (deep, rows), 0) == high, by_high, 0.0), axis=0, keepdims=True
    )
    shard_hot = jnp.where(lax.broadcasted_iota(i32, (wide, rows), 0) == target, kept, 0.0)
    shard_bf = shard_hot.astype(bf16)
    earlier = (
        lax.broadcasted_iota(i32, (rows, rows), 0) < lax.broadcasted_iota(i32, (rows, rows), 1)
    ).astype(f32).astype(bf16)
    running = jnp.dot(shard_bf, earlier, preferred_element_type=f32)
    rank = jnp.sum(shard_hot * running, axis=0, keepdims=True).astype(i32)
    slot_s[...] = jnp.where(kept > 0.5, target * cap + rank, -1)

    emb_copy.wait()

    def fill(k):
        a, b = place(owners, subs, k)
        t = a * subs + b
        hot = (slot_s[...] == t * cap + lax.broadcasted_iota(i32, (cap, rows), 0)).astype(f32).astype(bf16)
        send[k] = jnp.dot(hot, emb[...], preferred_element_type=f32).astype(bf16)

    def row_copy(k, source):
        a, b = place(owners, subs, k)
        return pltpu.make_async_remote_copy(
            src_ref=send.at[k], dst_ref=rows_ref.at[source],
            send_sem=send_sem.at[k], recv_sem=recv_sem.at[source],
            device_id={"owners": a, "sub": b}, device_id_type=MESH,
        )

    def meta_copy(k, source):
        a, b = place(owners, subs, k)
        return pltpu.make_async_remote_copy(
            src_ref=meta.at[k], dst_ref=got.at[source],
            send_sem=meta_send.at[k], recv_sem=meta_recv.at[source],
            device_id={"owners": a, "sub": b}, device_id_type=MESH,
        )

    def step(k, c):
        fill(k)
        row_copy(k - 1, own).start()
        return c

    fill(0)
    fill(1)
    pl.semaphore_wait(barrier, shards - 1)
    row_copy(0, own).start()
    lax.fori_loop(2, early, step, 0)

    square = emb[...].astype(f32)
    square = square * square
    square_hi = square.astype(bf16)
    square_lo = (square - square_hi.astype(f32)).astype(bf16)
    ones = jnp.ones((8, width), bf16)
    total = lax.dot_general(ones, square_hi, CROSS, preferred_element_type=f32)
    total = total + lax.dot_general(ones, square_lo, CROSS, preferred_element_type=f32)
    inverse_row = lax.rsqrt(total[0:1] + 1e-06)
    table_copy.wait()
    given = jnp.zeros((1, rows), f32)
    others = jnp.full((1, rows), -1e30, f32)
    for lo in range(0, classes, 128):
        n = min(128, classes - lo)
        part = table[lo : lo + n, :]
        part_f = part.astype(f32)
        inverse_class = lax.rsqrt(jnp.sum(part_f * part_f, axis=1, keepdims=True) + 1e-06)
        scaled = lax.dot_general(part, emb[...], CROSS, preferred_element_type=f32) * inverse_class
        match = lax.broadcasted_iota(i32, (n, rows), 0) + lo == near
        given = given + jnp.sum(jnp.where(match, scaled, 0.0), axis=0, keepdims=True)
        others = jnp.maximum(others, jnp.max(jnp.where(match, -1e30, scaled), axis=0, keepdims=True))
    margin = (20.0 * (given * inverse_row - others * inverse_row)).astype(bf16).astype(f32)
    rank_hot = (lax.broadcasted_iota(i32, (spots.shape[1], rows), 0) == rank).astype(f32).astype(bf16)
    spots[...] = lax.dot_general((shard_hot * margin).astype(bf16), rank_hot, CROSS, preferred_element_type=f32)
    counts = lax.dot_general(jnp.ones((8, rows), bf16), shard_bf, CROSS, preferred_element_type=f32)[0:1]

    def fill_meta(k, c):
        a, b = place(owners, subs, k)
        meta[k, 0:1, :] = spots[pl.ds(a * subs + b, 1), :]
        meta[k, 1:2, :] = counts
        return c

    lax.fori_loop(0, shards - 1, fill_meta, 0)
    got[own, 0:1, :] = spots[pl.ds(own, 1), :]
    got[own, 1:2, :] = counts

    lax.fori_loop(early, early + 1, step, 0)

    def send_meta(k, c):
        meta_copy(k, own).start()
        return c

    lax.fori_loop(0, shards - 1, send_meta, 0)
    lax.fori_loop(early + 1, shards, step, 0)
    own_copy = pltpu.make_async_copy(send.at[shards - 1], rows_ref.at[own], own_sem)
    own_copy.start()

    def take_meta(k, c):
        source = (own + 1 + k) % shards
        meta_copy(k, source).wait_recv()
        return c

    lax.fori_loop(0, shards - 1, take_meta, 0)

    def lay(s, c):
        scores_s[pl.ds(s, 1), :] = got[s, 0:1, :]
        counts_s[pl.ds(s, 1), :] = got[s, 1:2, :]
        return c

    lax.fori_loop(0, shards, lay, 0)
    table_counts = counts_s[...]
    totals_ref[...] = jnp.sum(table_counts, axis=0, keepdims=True).astype(i32)
    below = (
        lax.broadcasted_iota(i32, (shards, shards), 1) < lax.broadcasted_iota(i32, (shards, shards), 0)
    ).astype(f32)
    before = jnp.dot(below, table_counts, preferred_element_type=f32, precision=lax.Precision.HIGHEST)
    mine = lax.broadcasted_iota(i32, (shards, wide), 1) == own
    count_col = jnp.sum(jnp.where(mine, table_counts, 0.0), axis=1, keepdims=True).astype(i32)
    before_col = jnp.sum(jnp.where(mine, before, 0.0), axis=1, keepdims=True).astype(i32)
    offset = lax.broadcasted_iota(i32, (shards, slots), 1) - cap * lax.broadcasted_iota(i32, (shards, slots), 0)
    inside = (offset >= 0) & (offset < cap)
    spot = jnp.sum(jnp.where(inside, offset, 0), axis=0, keepdims=True)
    filled = jnp.where(offset < count_col, before_col + offset, -1)
    position_ref[...] = jnp.sum(jnp.where(inside, filled, 0), axis=0, keepdims=True)
    spread = (lax.broadcasted_iota(i32, (wide, slots), 0) == spot).astype(f32).astype(bf16)
    flat = jnp.dot(scores_s[...].astype(bf16), spread, preferred_element_type=f32)
    score_ref[...] = jnp.sum(jnp.where(inside, flat, 0.0), axis=0, keepdims=True).astype(score_ref.dtype)

    def finish(k, c):
        source = (own + 1 + k) % shards
        row_copy(k, source).wait_recv()
        row_copy(k, own).wait_send()
        meta_copy(k, own).wait_send()
        return c

    lax.fori_loop(0, shards - 1, finish, 0)
    own_copy.wait()


def quick_kernel(groups, owners, subs, cap, base, depth, near_hbm, keep_hbm, dest_hbm, emb_hbm, table_hbm,
                 rows_ref, score_ref, position_ref, totals_ref, flag_ref,
                 near_ref, keep_ref, dest_ref, emb, table, keep2, earlier, send, spare, spill, news, heard, told, scored,
                 heard_s, scores_s, slot_s, verdict,
                 in_sem, send_sem, recv_sem, news_send, news_recv, score_send, score_recv, spare_send, spare_recv,
                 relay_send, relay_recv, flag_send, flag_recv, own_sem):
    f32, bf16, i32 = jnp.float32, jnp.bfloat16, jnp.int32
    shards = owners * subs
    rows, width = emb.shape
    classes = table.shape[0]
    wide = news.shape[2]
    lead = wide - shards
    slots = shards * cap
    g, o, z = lax.axis_index("groups"), lax.axis_index("owners"), lax.axis_index("sub")
    own = o * subs + z
    peers = [(o + 1 + i) % owners for i in range(owners)]
    planes = [place(owners, subs, j * owners)[1] for j in range(subs)]

    small = [
        pltpu.make_async_copy(near_hbm, near_ref, in_sem.at[2]),
        pltpu.make_async_copy(keep_hbm, keep_ref, in_sem.at[3]),
        pltpu.make_async_copy(dest_hbm, dest_ref, in_sem.at[4]),
    ]
    for copy in small:
        copy.start()
    emb_copy = pltpu.make_async_copy(emb_hbm, emb, in_sem.at[0])
    emb_copy.start()
    table_copy = pltpu.make_async_copy(table_hbm, table, in_sem.at[1])
    table_copy.start()

    def device(j, i):
        return {"owners": peers[i], "sub": planes[j]}

    pairs = [(j, i) for j in range(subs) for i in range(owners)][: shards - 1]
    barrier = pltpu.get_barrier_semaphore()
    for j, i in pairs:
        pl.semaphore_signal(barrier, inc=1, device_id=device(j, i), device_id_type=MESH)
    for i in range(1, groups):
        pl.semaphore_signal(barrier, inc=1, device_id={"groups": (g + i) % groups}, device_id_type=MESH)

    earlier[...] = (
        lax.broadcasted_iota(i32, (rows, rows), 0) < lax.broadcasted_iota(i32, (rows, rows), 1)
    ).astype(f32).astype(bf16)
    keep2[...] = jnp.zeros_like(keep2)
    for copy in small:
        copy.wait()
    near = near_ref[...]
    target = dest_ref[...]
    for h in range(up(classes, 128) // 128):
        n = min(128, classes - h * 128)
        keep2[h : h + 1, :n] = keep_ref[:, h * 128 : h * 128 + n].astype(f32)
    deep = keep2.shape[0]
    high = near // 128
    low = near - high * 128
    low_hot = (lax.broadcasted_iota(i32, (128, rows), 0) == low).astype(f32).astype(bf16)
    by_high = jnp.dot(keep2[...].astype(bf16), low_hot, preferred_element_type=f32)
    kept = jnp.sum(
        jnp.where(lax.broadcasted_iota(i32, (deep, rows), 0) == high, by_high, 0.0), axis=0, keepdims=True
    )
    shard_hot = jnp.where(lax.broadcasted_iota(i32, (up(shards, 8), rows), 0) == target, kept, 0.0)
    running = jnp.dot(shard_hot.astype(bf16), earlier[...], preferred_element_type=f32)
    rank = jnp.sum(shard_hot * running, axis=0, keepdims=True).astype(i32)
    slot_s[...] = jnp.where(kept > 0.5, target * cap + rank, -1)

    ahead = target - target // subs * subs - z
    ahead = jnp.where(ahead < 0, ahead + subs, ahead)
    over = (kept > 0.5) & (rank >= base) & (ahead > 0)
    plane_hot = jnp.where((lax.broadcasted_iota(i32, (up(subs, 8), rows), 0) == ahead) & over, 1.0, 0.0)
    before_it = jnp.dot(plane_hot.astype(bf16), earlier[...], preferred_element_type=f32)
    spot = jnp.sum(plane_hot * before_it, axis=0, keepdims=True).astype(i32)
    fits = over & (spot < depth)
    nth = jnp.where(fits, spot + 1, 0).astype(f32)

    rank_hot = (lax.broadcasted_iota(i32, (wide, rows), 0) == rank).astype(f32).astype(bf16)
    count_hot = jnp.where(lax.broadcasted_iota(i32, (wide, rows), 0) == target + lead, kept, 0.0).astype(bf16)
    notes = lax.dot_general((shard_hot * nth).astype(bf16), rank_hot, CROSS, preferred_element_type=f32)
    notes = notes + lax.dot_general(
        jnp.ones((up(shards, 8), rows), bf16), count_hot, CROSS, preferred_element_type=f32
    )
    for t in range(shards):
        news[t] = notes[t : t + 1]
    heard[own] = news[own]

    emb_copy.wait()

    seat = jnp.where(fits, (ahead - 1) * depth + spot, -1)
    hot = (lax.broadcasted_iota(i32, ((subs - 1) * depth, rows), 0) == seat).astype(f32).astype(bf16)
    packed = jnp.dot(hot, emb[...], preferred_element_type=f32).astype(bf16)
    for d in range(subs - 1):
        spare[d] = packed[d * depth : (d + 1) * depth]

    def fill(j, n):
        slot = slot_s[...] - planes[j] * cap
        hot = jnp.concatenate([
            (slot - a * subs * cap == lax.broadcasted_iota(i32, (n, rows), 0)).astype(f32).astype(bf16) for a in peers
        ])
        block = jnp.dot(hot, emb[...], preferred_element_type=f32).astype(bf16)
        for i in range(owners):
            send[j * owners + i, :n] = block[i * n : (i + 1) * n]

    def row_copy(j, i, n):
        k = j * owners + i
        return pltpu.make_async_remote_copy(
            src_ref=send.at[k, :n], dst_ref=rows_ref.at[own, :n],
            send_sem=send_sem.at[k], recv_sem=recv_sem.at[own],
            device_id=device(j, i), device_id_type=MESH,
        )

    def row_arrival(j, i, n):
        source = peers[i] * subs + planes[j]
        return pltpu.make_async_remote_copy(
            src_ref=send.at[0, :n], dst_ref=rows_ref.at[source, :n],
            send_sem=send_sem.at[0], recv_sem=recv_sem.at[source],
            device_id=device(j, i), device_id_type=MESH,
        )

    def note_copy(j, i, ref, landing, out_sem, in_sem, source):
        t = peers[i] * subs + planes[j]
        return pltpu.make_async_remote_copy(
            src_ref=ref.at[t], dst_ref=landing.at[source],
            send_sem=out_sem.at[t], recv_sem=in_sem.at[source],
            device_id=device(j, i), device_id_type=MESH,
        )

    def news_copy(j, i, source):
        return note_copy(j, i, news, heard, news_send, news_recv, source)

    def score_copy(j, i, source):
        return note_copy(j, i, told, scored, score_send, score_recv, source)

    ways = [(b - z + subs) % subs for b in planes[: subs - 1]]

    def spare_copy(j, arrival=False):
        slot = ways[j] - 1 if arrival else subs - 1 - ways[j]
        return pltpu.make_async_remote_copy(
            src_ref=spare.at[ways[j] - 1], dst_ref=spill.at[o, slot],
            send_sem=spare_send.at[ways[j] - 1], recv_sem=spare_recv.at[slot],
            device_id={"owners": o, "sub": planes[j]}, device_id_type=MESH,
        )

    def relay_copy(i, j, source):
        slot = ways[j] - 1
        return pltpu.make_async_remote_copy(
            src_ref=spill.at[source, slot], dst_ref=spill.at[source, slot],
            send_sem=relay_send.at[i, slot], recv_sem=relay_recv.at[source, slot],
            device_id={"owners": peers[i], "sub": z}, device_id_type=MESH,
        )

    def flag_copy(i, source):
        return pltpu.make_async_remote_copy(
            src_ref=verdict.at[g], dst_ref=verdict.at[source],
            send_sem=flag_send.at[i], recv_sem=flag_recv.at[source],
            device_id={"groups": (g + i) % groups}, device_id_type=MESH,
        )

    pl.semaphore_wait(barrier, shards - 1 + groups - 1)
    for j in range(subs - 1):
        spare_copy(j).start()
    for j, i in pairs:
        news_copy(j, i, own).start()
    fill(0, base)
    for i in range(owners):
        row_copy(0, i, base).start()
    fill(subs - 1, cap)
    for i in range(owners - 1):
        row_copy(subs - 1, i, cap).start()
    own_copy = pltpu.make_async_copy(send.at[shards - 1], rows_ref.at[own], own_sem)
    own_copy.start()
    square = emb[...].astype(f32)
    square = square * square
    square_hi = square.astype(bf16)
    square_lo = (square - square_hi.astype(f32)).astype(bf16)
    ones = jnp.ones((8, width), bf16)
    total = lax.dot_general(ones, square_hi, CROSS, preferred_element_type=f32)
    total = total + lax.dot_general(ones, square_lo, CROSS, preferred_element_type=f32)
    inverse_row = lax.rsqrt(total[0:1] + 1e-06)
    table_copy.wait()
    given = jnp.zeros((1, rows), f32)
    others = jnp.full((1, rows), -1e30, f32)
    for lo in range(0, classes, 128):
        n = min(128, classes - lo)
        part = table[lo : lo + n, :]
        part_f = part.astype(f32)
        inverse_class = lax.rsqrt(jnp.sum(part_f * part_f, axis=1, keepdims=True) + 1e-06)
        scaled = lax.dot_general(part, emb[...], CROSS, preferred_element_type=f32) * inverse_class
        match = lax.broadcasted_iota(i32, (n, rows), 0) + lo == near
        given = given + jnp.sum(jnp.where(match, scaled, 0.0), axis=0, keepdims=True)
        others = jnp.maximum(others, jnp.max(jnp.where(match, -1e30, scaled), axis=0, keepdims=True))
    margin = (20.0 * (given * inverse_row - others * inverse_row)).astype(bf16).astype(f32)
    rank_hot = (lax.broadcasted_iota(i32, (wide, rows), 0) == rank).astype(f32).astype(bf16)
    marks = lax.dot_general((shard_hot * margin).astype(bf16), rank_hot, CROSS, preferred_element_type=f32)
    for t in range(shards):
        told[t] = marks[t : t + 1]
    scored[own] = told[own]
    fill(1, base)
    for j, i in pairs:
        score_copy(j, i, own).start()
    for j in range(1, subs - 1):
        if j > 1:
            fill(j, base)
        for i in range(owners):
            row_copy(j, i, base).start()

    for j, i in pairs:
        news_copy(j, i, peers[i] * subs + planes[j]).wait_recv()
    for t in range(shards):
        heard_s[t : t + 1, :] = heard[t]
    counts = jnp.where(lax.broadcasted_iota(i32, (shards, wide), 1) >= lead, heard_s[...], 0.0)
    row_i, col_i = lax.broadcasted_iota(i32, (wide, wide), 0), lax.broadcasted_iota(i32, (wide, wide), 1)
    plane = ((row_i >= lead) & ((row_i - lead) % subs == col_i)).astype(f32)
    past = jnp.dot(jnp.maximum(counts - base, 0.0), plane, preferred_element_type=f32)
    away = lax.broadcasted_iota(i32, (shards, wide), 0) % subs != lax.broadcasted_iota(i32, (shards, wide), 1)
    most = jnp.max(jnp.max(jnp.where(away, past, 0.0), axis=1, keepdims=True), axis=0, keepdims=True)
    verdict[g] = jnp.broadcast_to(most, (1, wide))

    totals_ref[...] = jnp.sum(counts, axis=0, keepdims=True)[:, lead:].astype(i32)
    below = (
        lax.broadcasted_iota(i32, (shards, shards), 1) < lax.broadcasted_iota(i32, (shards, shards), 0)
    ).astype(f32)
    before = jnp.dot(below, counts, preferred_element_type=f32, precision=lax.Precision.HIGHEST)
    mine = lax.broadcasted_iota(i32, (shards, wide), 1) == own + lead
    count_col = jnp.sum(jnp.where(mine, counts, 0.0), axis=1, keepdims=True).astype(i32)
    before_col = jnp.sum(jnp.where(mine, before, 0.0), axis=1, keepdims=True).astype(i32)
    for i in range(1, groups):
        flag_copy(i, g).start()
    offset = lax.broadcasted_iota(i32, (shards, slots), 1) - cap * lax.broadcasted_iota(i32, (shards, slots), 0)
    inside = (offset >= 0) & (offset < cap)
    nook = jnp.sum(jnp.where(inside, offset, 0), axis=0, keepdims=True)
    filled = jnp.where(offset < count_col, before_col + offset, -1)
    position_ref[...] = jnp.sum(jnp.where(inside, filled, 0), axis=0, keepdims=True)

    def merge(a, j):
        s = a * subs + planes[j]
        nth_row = heard[s][:, base:cap].astype(i32)
        pick = (lax.broadcasted_iota(i32, (depth, cap - base), 0) + 1 == nth_row).astype(f32).astype(bf16)
        rest = lax.dot_general(pick, spill[a, ways[j] - 1], DOWN, preferred_element_type=f32)
        rows_ref[s, base:cap] = rest.astype(bf16)

    order = [*range(1, subs - 1), 0]
    for j in order:
        spare_copy(j, True).wait_recv()
        for i in range(owners - 1):
            relay_copy(i, j, o).start()
        merge(o, j)
    for i in range(1, groups):
        flag_copy(i, (g + groups - i) % groups).wait_recv()
    flag_ref[0] = (jnp.max(verdict[...]) > depth).astype(i32)
    for j in order:
        for i in range(owners - 1):
            relay_copy(i, j, peers[i]).wait_recv()
            merge(peers[i], j)

    for j, i in pairs:
        score_copy(j, i, peers[i] * subs + planes[j]).wait_recv()
    for t in range(shards):
        scores_s[t : t + 1, :] = scored[t]
    spread = (lax.broadcasted_iota(i32, (wide, slots), 0) == nook).astype(f32).astype(bf16)
    flat = jnp.dot(scores_s[...].astype(bf16), spread, preferred_element_type=f32)
    score_ref[...] = jnp.sum(jnp.where(inside, flat, 0.0), axis=0, keepdims=True).astype(score_ref.dtype)

    for i in range(1, groups):
        flag_copy(i, g).wait_send()
    for j in range(subs - 1):
        spare_copy(j).wait_send()
    for j in range(subs - 1):
        for i in range(owners - 1):
            relay_copy(i, j, o).wait_send()
    own_copy.wait()
    for j, i in pairs:
        news_copy(j, i, own).wait_send()
        score_copy(j, i, own).wait_send()
        row_copy(j, i, base if j < subs - 1 else cap).wait_send()
    for j, i in pairs:
        row_arrival(j, i, base if j < subs - 1 else cap).wait_recv()


def plain(call, embeddings, class_table, nearest, keep_class, destination):
    owners, subs = lax.axis_size("owners"), lax.axis_size("sub")
    shards = owners * subs
    rows, width = embeddings.shape
    classes = class_table.shape[0]
    cap = 3 * rows // (2 * shards)
    wide = up(max(shards, cap), 128)
    early = max(2, shards // 4)
    vmem = pl.BlockSpec(memory_space=pltpu.VMEM)
    hbm = pl.BlockSpec(memory_space=pl.ANY)
    f32, bf16, i32 = jnp.float32, jnp.bfloat16, jnp.int32
    dma = pltpu.SemaphoreType.DMA
    return pl.pallas_call(
        functools.partial(kernel, owners, subs, cap, early),
        out_shape=(
            pltpu.VMEM((shards, cap, width), bf16),
            pltpu.VMEM((1, shards * cap), f32),
            pltpu.VMEM((1, shards * cap), i32),
            pltpu.VMEM((1, wide), i32),
        ),
        in_specs=[hbm] * 5,
        out_specs=(vmem,) * 4,
        scratch_shapes=[
            pltpu.VMEM((1, rows), i32),
            pltpu.VMEM((1, classes), i32),
            pltpu.VMEM((1, rows), i32),
            pltpu.VMEM((rows, width), bf16),
            pltpu.VMEM((classes, width), bf16),
            pltpu.VMEM((up(up(classes, 128) // 128, 8), 128), f32),
            pltpu.VMEM((shards, cap, width), bf16),
            pltpu.VMEM((shards, 2, wide), f32),
            pltpu.VMEM((shards, 2, wide), f32),
            pltpu.VMEM((wide, wide), f32),
            pltpu.VMEM((shards, wide), f32),
            pltpu.VMEM((shards, wide), f32),
            pltpu.VMEM((1, rows), i32),
            dma((5,)),
            dma((shards,)),
            dma((shards,)),
            dma((shards,)),
            dma((shards,)),
            dma,
        ],
        compiler_params=pltpu.CompilerParams(collective_id=call, has_side_effects=True),
    )(
        nearest.reshape(1, rows),
        keep_class.reshape(1, classes),
        destination.reshape(1, rows),
        embeddings,
        class_table,
    )


def quick(base, depth, embeddings, class_table, nearest, keep_class, destination):
    groups, owners, subs = lax.axis_size("groups"), lax.axis_size("owners"), lax.axis_size("sub")
    shards = owners * subs
    rows, width = embeddings.shape
    classes = class_table.shape[0]
    cap = 3 * rows // (2 * shards)
    wide = up(shards + cap, 128)
    vmem = pl.BlockSpec(memory_space=pltpu.VMEM)
    hbm = pl.BlockSpec(memory_space=pl.ANY)
    f32, bf16, i32 = jnp.float32, jnp.bfloat16, jnp.int32
    dma = pltpu.SemaphoreType.DMA
    return pl.pallas_call(
        functools.partial(quick_kernel, groups, owners, subs, cap, base, depth),
        out_shape=(
            pltpu.VMEM((shards, cap, width), bf16),
            pltpu.VMEM((1, shards * cap), f32),
            pltpu.VMEM((1, shards * cap), i32),
            pltpu.VMEM((1, shards), i32),
            pltpu.SMEM((1,), i32),
        ),
        in_specs=[hbm] * 5,
        out_specs=(vmem,) * 4 + (pl.BlockSpec(memory_space=pltpu.SMEM),),
        scratch_shapes=[
            pltpu.VMEM((1, rows), i32),
            pltpu.VMEM((1, classes), i32),
            pltpu.VMEM((1, rows), i32),
            pltpu.VMEM((rows, width), bf16),
            pltpu.VMEM((classes, width), bf16),
            pltpu.VMEM((up(up(classes, 128) // 128, 8), 128), f32),
            pltpu.VMEM((rows, rows), bf16),
            pltpu.VMEM((shards, cap, width), bf16),
            pltpu.VMEM((subs - 1, depth, width), bf16),
            pltpu.VMEM((owners, subs - 1, depth, width), bf16),
            pltpu.VMEM((shards, 1, wide), f32),
            pltpu.VMEM((shards, 1, wide), f32),
            pltpu.VMEM((shards, 1, wide), f32),
            pltpu.VMEM((shards, 1, wide), f32),
            pltpu.VMEM((shards, wide), f32),
            pltpu.VMEM((shards, wide), f32),
            pltpu.VMEM((1, rows), i32),
            pltpu.VMEM((groups, 1, wide), f32),
            dma((5,)),
            dma((shards,)),
            dma((shards,)),
            dma((shards,)),
            dma((shards,)),
            dma((shards,)),
            dma((shards,)),
            dma((subs - 1,)),
            dma((subs - 1,)),
            dma((owners, subs - 1)),
            dma((owners, subs - 1)),
            dma((groups,)),
            dma((groups,)),
            dma,
        ],
        compiler_params=pltpu.CompilerParams(collective_id=0, has_side_effects=True),
    )(
        nearest.reshape(1, rows),
        keep_class.reshape(1, classes),
        destination.reshape(1, rows),
        embeddings,
        class_table,
    )


def close(got_rows, score, position, totals):
    shards, cap, width = got_rows.shape
    wide = totals.shape[1]
    vmem = pl.BlockSpec(memory_space=pltpu.VMEM)
    hbm = pl.BlockSpec(memory_space=pl.ANY)
    bf16, i32 = jnp.bfloat16, jnp.int32
    dma = pltpu.SemaphoreType.DMA
    small = [pltpu.with_memory_space_constraint(x, pltpu.VMEM) for x in (got_rows, score, position, totals)]
    rows_out, score_out, position_out, totals_out = pl.pallas_call(
        finish_kernel,
        out_shape=(
            jax.ShapeDtypeStruct((shards, cap, width), bf16),
            jax.ShapeDtypeStruct((shards * cap,), bf16),
            jax.ShapeDtypeStruct((shards * cap,), i32),
            jax.ShapeDtypeStruct((wide,), i32),
        ),
        in_specs=[vmem] * 4,
        out_specs=(hbm,) * 4,
        scratch_shapes=[
            pltpu.VMEM((shards * cap,), bf16),
            pltpu.VMEM((shards * cap,), i32),
            pltpu.VMEM((wide,), i32),
            dma((4,)),
        ],
    )(*small)
    return rows_out.reshape(shards * cap, width), score_out, position_out, totals_out[:shards]


def on_device(*args):
    rows = args[0].shape[0]
    subs, shards = lax.axis_size("sub"), lax.axis_size("owners") * lax.axis_size("sub")
    cap = 3 * rows // (2 * shards)
    base, depth = 2 * cap // 3, cap // 2
    if subs < 2 or shards % 8 or base % 16 or cap % 16 or depth % 8:
        return close(*plain(0, *args))
    *packed, flag = quick(base, depth, *args)

    def fast(inputs, results):
        return close(*results)

    def slow(inputs, results):
        return close(*plain(1, *inputs))

    return lax.cond(flag.reshape(()) > 0, slow, fast, args, tuple(packed))


def solution(mesh):
    in_specs = (
        P(("groups", "owners", "sub"), None),
        P(),
        P(("groups", "owners", "sub")),
        P(),
        P(("groups", "owners", "sub"), None),
    )
    out_specs = (
        P(("groups", "owners", "sub"), None),
        P(("groups", "owners", "sub")),
        P(("groups", "owners", "sub")),
        P("groups"),
    )
    return jax.shard_map(
        on_device, mesh=mesh, in_specs=in_specs, out_specs=out_specs, check_vma=False
    )
```

```python
import functools

import jax
import jax.numpy as jnp
from jax import lax
from jax.experimental import pallas as pl
from jax.experimental.pallas import tpu as pltpu
from jax.sharding import PartitionSpec as P

MESH = pl.DeviceIdType.MESH
CROSS = (((1,), (1,)), ((), ()))
DOWN = (((0,), (0,)), ((), ()))


def up(value, step):
    return (value + step - 1) // step * step


def place(owners, subs, k):
    o, z = lax.axis_index("owners"), lax.axis_index("sub")
    upper = (2 * z) // subs
    toward = upper * z + (1 - upper) * (subs - 1 - z)
    j = k // owners
    first = 1 - (j + subs - 1) // subs
    past = (j + subs - toward) // subs
    far = first * toward + (1 - first) * (j + past)
    to_sub = (z + far * (1 - 2 * upper) + subs) % subs
    to_owner = (o + 1 + k % owners) % owners
    return to_owner, to_sub


def finish_kernel(rows_ref, score_ref, position_ref, totals_ref, rows_out, score_out, position_out, totals_out,
                  score_s, position_s, totals_s, sem):
    copies = [pltpu.make_async_copy(rows_ref, rows_out, sem.at[0])]
    copies[0].start()
    position_s[...] = position_ref[...].reshape(position_s.shape)
    totals_s[...] = totals_ref[...].reshape(totals_s.shape)
    score_s[...] = score_ref[...].reshape(score_s.shape).astype(score_s.dtype)
    for i, (inner, outer) in enumerate(((position_s, position_out), (totals_s, totals_out), (score_s, score_out))):
        copies.append(pltpu.make_async_copy(inner, outer, sem.at[i + 1]))
        copies[-1].start()
    for copy in copies:
        copy.wait()


def kernel(owners, subs, cap, early, near_hbm, keep_hbm, dest_hbm, emb_hbm, table_hbm,
           rows_ref, score_ref, position_ref, totals_ref,
           near_ref, keep_ref, dest_ref, emb, table, keep2, send, meta, got, spots, counts_s, scores_s, slot_s,
           in_sem, send_sem, recv_sem, meta_send, meta_recv, own_sem):
    f32, bf16, i32 = jnp.float32, jnp.bfloat16, jnp.int32
    shards = owners * subs
    rows, width = emb.shape
    classes = table.shape[0]
    wide = meta.shape[2]
    slots = shards * cap
    o, z = lax.axis_index("owners"), lax.axis_index("sub")
    own = o * subs + z

    small = [
        pltpu.make_async_copy(near_hbm, near_ref, in_sem.at[2]),
        pltpu.make_async_copy(keep_hbm, keep_ref, in_sem.at[3]),
        pltpu.make_async_copy(dest_hbm, dest_ref, in_sem.at[4]),
    ]
    for copy in small:
        copy.start()
    emb_copy = pltpu.make_async_copy(emb_hbm, emb, in_sem.at[0])
    emb_copy.start()
    table_copy = pltpu.make_async_copy(table_hbm, table, in_sem.at[1])
    table_copy.start()

    barrier = pltpu.get_barrier_semaphore()

    def greet(k, c):
        a, b = place(owners, subs, k)
        pl.semaphore_signal(barrier, inc=1, device_id={"owners": a, "sub": b}, device_id_type=MESH)
        return c

    lax.fori_loop(0, shards - 1, greet, 0)

    for copy in small:
        copy.wait()
    near = near_ref[...]
    target = dest_ref[...]
    keep2[...] = jnp.zeros_like(keep2)
    for h in range(up(classes, 128) // 128):
        n = min(128, classes - h * 128)
        keep2[h : h + 1, :n] = keep_ref[:, h * 128 : h * 128 + n].astype(f32)
    deep = keep2.shape[0]
    high = near // 128
    low = near - high * 128
    low_hot = (lax.broadcasted_iota(i32, (128, rows), 0) == low).astype(f32).astype(bf16)
    by_high = jnp.dot(keep2[...].astype(bf16), low_hot, preferred_element_type=f32)
    kept = jnp.sum(
        jnp.where(lax.broadcasted_iota(i32, (deep, rows), 0) == high, by_high, 0.0), axis=0, keepdims=True
    )
    shard_hot = jnp.where(lax.broadcasted_iota(i32, (wide, rows), 0) == target, kept, 0.0)
    shard_bf = shard_hot.astype(bf16)
    earlier = (
        lax.broadcasted_iota(i32, (rows, rows), 0) < lax.broadcasted_iota(i32, (rows, rows), 1)
    ).astype(f32).astype(bf16)
    running = jnp.dot(shard_bf, earlier, preferred_element_type=f32)
    rank = jnp.sum(shard_hot * running, axis=0, keepdims=True).astype(i32)
    slot_s[...] = jnp.where(kept > 0.5, target * cap + rank, -1)

    emb_copy.wait()

    def fill(k):
        a, b = place(owners, subs, k)
        t = a * subs + b
        hot = (slot_s[...] == t * cap + lax.broadcasted_iota(i32, (cap, rows), 0)).astype(f32).astype(bf16)
        send[k] = jnp.dot(hot, emb[...], preferred_element_type=f32).astype(bf16)

    def row_copy(k, source):
        a, b = place(owners, subs, k)
        return pltpu.make_async_remote_copy(
            src_ref=send.at[k], dst_ref=rows_ref.at[source],
            send_sem=send_sem.at[k], recv_sem=recv_sem.at[source],
            device_id={"owners": a, "sub": b}, device_id_type=MESH,
        )

    def meta_copy(k, source):
        a, b = place(owners, subs, k)
        return pltpu.make_async_remote_copy(
            src_ref=meta.at[k], dst_ref=got.at[source],
            send_sem=meta_send.at[k], recv_sem=meta_recv.at[source],
            device_id={"owners": a, "sub": b}, device_id_type=MESH,
        )

    def step(k, c):
        fill(k)
        row_copy(k - 1, own).start()
        return c

    fill(0)
    fill(1)
    pl.semaphore_wait(barrier, shards - 1)
    row_copy(0, own).start()
    lax.fori_loop(2, early, step, 0)

    square = emb[...].astype(f32)
    square = square * square
    square_hi = square.astype(bf16)
    square_lo = (square - square_hi.astype(f32)).astype(bf16)
    ones = jnp.ones((8, width), bf16)
    total = lax.dot_general(ones, square_hi, CROSS, preferred_element_type=f32)
    total = total + lax.dot_general(ones, square_lo, CROSS, preferred_element_type=f32)
    inverse_row = lax.rsqrt(total[0:1] + 1e-06)
    table_copy.wait()
    given = jnp.zeros((1, rows), f32)
    others = jnp.full((1, rows), -1e30, f32)
    for lo in range(0, classes, 128):
        n = min(128, classes - lo)
        part = table[lo : lo + n, :]
        part_f = part.astype(f32)
        inverse_class = lax.rsqrt(jnp.sum(part_f * part_f, axis=1, keepdims=True) + 1e-06)
        scaled = lax.dot_general(part, emb[...], CROSS, preferred_element_type=f32) * inverse_class
        match = lax.broadcasted_iota(i32, (n, rows), 0) + lo == near
        given = given + jnp.sum(jnp.where(match, scaled, 0.0), axis=0, keepdims=True)
        others = jnp.maximum(others, jnp.max(jnp.where(match, -1e30, scaled), axis=0, keepdims=True))
    margin = (20.0 * (given * inverse_row - others * inverse_row)).astype(bf16).astype(f32)
    rank_hot = (lax.broadcasted_iota(i32, (spots.shape[1], rows), 0) == rank).astype(f32).astype(bf16)
    spots[...] = lax.dot_general((shard_hot * margin).astype(bf16), rank_hot, CROSS, preferred_element_type=f32)
    counts = lax.dot_general(jnp.ones((8, rows), bf16), shard_bf, CROSS, preferred_element_type=f32)[0:1]

    def fill_meta(k, c):
        a, b = place(owners, subs, k)
        meta[k, 0:1, :] = spots[pl.ds(a * subs + b, 1), :]
        meta[k, 1:2, :] = counts
        return c

    lax.fori_loop(0, shards - 1, fill_meta, 0)
    got[own, 0:1, :] = spots[pl.ds(own, 1), :]
    got[own, 1:2, :] = counts

    lax.fori_loop(early, early + 1, step, 0)

    def send_meta(k, c):
        meta_copy(k, own).start()
        return c

    lax.fori_loop(0, shards - 1, send_meta, 0)
    lax.fori_loop(early + 1, shards, step, 0)
    own_copy = pltpu.make_async_copy(send.at[shards - 1], rows_ref.at[own], own_sem)
    own_copy.start()

    def take_meta(k, c):
        source = (own + 1 + k) % shards
        meta_copy(k, source).wait_recv()
        return c

    lax.fori_loop(0, shards - 1, take_meta, 0)

    def lay(s, c):
        scores_s[pl.ds(s, 1), :] = got[s, 0:1, :]
        counts_s[pl.ds(s, 1), :] = got[s, 1:2, :]
        return c

    lax.fori_loop(0, shards, lay, 0)
    table_counts = counts_s[...]
    totals_ref[...] = jnp.sum(table_counts, axis=0, keepdims=True).astype(i32)
    below = (
        lax.broadcasted_iota(i32, (shards, shards), 1) < lax.broadcasted_iota(i32, (shards, shards), 0)
    ).astype(f32)
    before = jnp.dot(below, table_counts, preferred_element_type=f32, precision=lax.Precision.HIGHEST)
    mine = lax.broadcasted_iota(i32, (shards, wide), 1) == own
    count_col = jnp.sum(jnp.where(mine, table_counts, 0.0), axis=1, keepdims=True).astype(i32)
    before_col = jnp.sum(jnp.where(mine, before, 0.0), axis=1, keepdims=True).astype(i32)
    offset = lax.broadcasted_iota(i32, (shards, slots), 1) - cap * lax.broadcasted_iota(i32, (shards, slots), 0)
    inside = (offset >= 0) & (offset < cap)
    spot = jnp.sum(jnp.where(inside, offset, 0), axis=0, keepdims=True)
    filled = jnp.where(offset < count_col, before_col + offset, -1)
    position_ref[...] = jnp.sum(jnp.where(inside, filled, 0), axis=0, keepdims=True)
    spread = (lax.broadcasted_iota(i32, (wide, slots), 0) == spot).astype(f32).astype(bf16)
    flat = jnp.dot(scores_s[...].astype(bf16), spread, preferred_element_type=f32)
    score_ref[...] = jnp.sum(jnp.where(inside, flat, 0.0), axis=0, keepdims=True).astype(score_ref.dtype)

    def finish(k, c):
        source = (own + 1 + k) % shards
        row_copy(k, source).wait_recv()
        row_copy(k, own).wait_send()
        meta_copy(k, own).wait_send()
        return c

    lax.fori_loop(0, shards - 1, finish, 0)
    own_copy.wait()


def quick_kernel(groups, owners, subs, cap, base, depth, near_hbm, keep_hbm, dest_hbm, emb_hbm, table_hbm,
                 rows_ref, score_ref, position_ref, totals_ref, flag_ref,
                 near_ref, keep_ref, dest_ref, emb, table, keep2, earlier, send, spare, spill, news, heard, told, scored,
                 heard_s, scores_s, slot_s, verdict,
                 in_sem, send_sem, recv_sem, news_send, news_recv, score_send, score_recv, spare_send, spare_recv,
                 relay_send, relay_recv, flag_send, flag_recv, own_sem):
    f32, bf16, i32 = jnp.float32, jnp.bfloat16, jnp.int32
    shards = owners * subs
    rows, width = emb.shape
    classes = table.shape[0]
    wide = news.shape[2]
    lead = wide - shards
    slots = shards * cap
    g, o, z = lax.axis_index("groups"), lax.axis_index("owners"), lax.axis_index("sub")
    own = o * subs + z
    peers = [(o + 1 + i) % owners for i in range(owners)]
    planes = [place(owners, subs, j * owners)[1] for j in range(subs)]

    small = [
        pltpu.make_async_copy(near_hbm, near_ref, in_sem.at[2]),
        pltpu.make_async_copy(keep_hbm, keep_ref, in_sem.at[3]),
        pltpu.make_async_copy(dest_hbm, dest_ref, in_sem.at[4]),
    ]
    for copy in small:
        copy.start()
    emb_copy = pltpu.make_async_copy(emb_hbm, emb, in_sem.at[0])
    emb_copy.start()
    table_copy = pltpu.make_async_copy(table_hbm, table, in_sem.at[1])
    table_copy.start()

    def device(j, i):
        return {"owners": peers[i], "sub": planes[j]}

    pairs = [(j, i) for j in range(subs) for i in range(owners)][: shards - 1]
    barrier = pltpu.get_barrier_semaphore()
    for j, i in pairs:
        pl.semaphore_signal(barrier, inc=1, device_id=device(j, i), device_id_type=MESH)
    for i in range(1, groups):
        pl.semaphore_signal(barrier, inc=1, device_id={"groups": (g + i) % groups}, device_id_type=MESH)

    earlier[...] = (
        lax.broadcasted_iota(i32, (rows, rows), 0) < lax.broadcasted_iota(i32, (rows, rows), 1)
    ).astype(f32).astype(bf16)
    keep2[...] = jnp.zeros_like(keep2)
    for copy in small:
        copy.wait()
    near = near_ref[...]
    target = dest_ref[...]
    for h in range(up(classes, 128) // 128):
        n = min(128, classes - h * 128)
        keep2[h : h + 1, :n] = keep_ref[:, h * 128 : h * 128 + n].astype(f32)
    deep = keep2.shape[0]
    high = near // 128
    low = near - high * 128
    low_hot = (lax.broadcasted_iota(i32, (128, rows), 0) == low).astype(f32).astype(bf16)
    by_high = jnp.dot(keep2[...].astype(bf16), low_hot, preferred_element_type=f32)
    kept = jnp.sum(
        jnp.where(lax.broadcasted_iota(i32, (deep, rows), 0) == high, by_high, 0.0), axis=0, keepdims=True
    )
    shard_hot = jnp.where(lax.broadcasted_iota(i32, (up(shards, 8), rows), 0) == target, kept, 0.0)
    running = jnp.dot(shard_hot.astype(bf16), earlier[...], preferred_element_type=f32)
    rank = jnp.sum(shard_hot * running, axis=0, keepdims=True).astype(i32)
    slot_s[...] = jnp.where(kept > 0.5, target * cap + rank, -1)

    ahead = target - target // subs * subs - z
    ahead = jnp.where(ahead < 0, ahead + subs, ahead)
    over = (kept > 0.5) & (rank >= base) & (ahead > 0)
    plane_hot = jnp.where((lax.broadcasted_iota(i32, (up(subs, 8), rows), 0) == ahead) & over, 1.0, 0.0)
    before_it = jnp.dot(plane_hot.astype(bf16), earlier[...], preferred_element_type=f32)
    spot = jnp.sum(plane_hot * before_it, axis=0, keepdims=True).astype(i32)
    fits = over & (spot < depth)
    nth = jnp.where(fits, spot + 1, 0).astype(f32)

    rank_hot = (lax.broadcasted_iota(i32, (wide, rows), 0) == rank).astype(f32).astype(bf16)
    count_hot = jnp.where(lax.broadcasted_iota(i32, (wide, rows), 0) == target + lead, kept, 0.0).astype(bf16)
    notes = lax.dot_general((shard_hot * nth).astype(bf16), rank_hot, CROSS, preferred_element_type=f32)
    notes = notes + lax.dot_general(
        jnp.ones((up(shards, 8), rows), bf16), count_hot, CROSS, preferred_element_type=f32
    )
    for t in range(shards):
        news[t] = notes[t : t + 1]
    heard[own] = news[own]

    emb_copy.wait()

    seat = jnp.where(fits, (ahead - 1) * depth + spot, -1)
    hot = (lax.broadcasted_iota(i32, ((subs - 1) * depth, rows), 0) == seat).astype(f32).astype(bf16)
    packed = jnp.dot(hot, emb[...], preferred_element_type=f32).astype(bf16)
    for d in range(subs - 1):
        spare[d] = packed[d * depth : (d + 1) * depth]

    def fill(j, n):
        slot = slot_s[...] - planes[j] * cap
        hot = jnp.concatenate([
            (slot - a * subs * cap == lax.broadcasted_iota(i32, (n, rows), 0)).astype(f32).astype(bf16) for a in peers
        ])
        block = jnp.dot(hot, emb[...], preferred_element_type=f32).astype(bf16)
        for i in range(owners):
            send[j * owners + i, :n] = block[i * n : (i + 1) * n]

    def row_copy(j, i, n):
        k = j * owners + i
        return pltpu.make_async_remote_copy(
            src_ref=send.at[k, :n], dst_ref=rows_ref.at[own, :n],
            send_sem=send_sem.at[k], recv_sem=recv_sem.at[own],
            device_id=device(j, i), device_id_type=MESH,
        )

    def row_arrival(j, i, n):
        source = peers[i] * subs + planes[j]
        return pltpu.make_async_remote_copy(
            src_ref=send.at[0, :n], dst_ref=rows_ref.at[source, :n],
            send_sem=send_sem.at[0], recv_sem=recv_sem.at[source],
            device_id=device(j, i), device_id_type=MESH,
        )

    def note_copy(j, i, ref, landing, out_sem, in_sem, source):
        t = peers[i] * subs + planes[j]
        return pltpu.make_async_remote_copy(
            src_ref=ref.at[t], dst_ref=landing.at[source],
            send_sem=out_sem.at[t], recv_sem=in_sem.at[source],
            device_id=device(j, i), device_id_type=MESH,
        )

    def news_copy(j, i, source):
        return note_copy(j, i, news, heard, news_send, news_recv, source)

    def score_copy(j, i, source):
        return note_copy(j, i, told, scored, score_send, score_recv, source)

    ways = [(b - z + subs) % subs for b in planes[: subs - 1]]

    def spare_copy(j, arrival=False):
        slot = ways[j] - 1 if arrival else subs - 1 - ways[j]
        return pltpu.make_async_remote_copy(
            src_ref=spare.at[ways[j] - 1], dst_ref=spill.at[o, slot],
            send_sem=spare_send.at[ways[j] - 1], recv_sem=spare_recv.at[slot],
            device_id={"owners": o, "sub": planes[j]}, device_id_type=MESH,
        )

    def relay_copy(i, j, source):
        slot = ways[j] - 1
        return pltpu.make_async_remote_copy(
            src_ref=spill.at[source, slot], dst_ref=spill.at[source, slot],
            send_sem=relay_send.at[i, slot], recv_sem=relay_recv.at[source, slot],
            device_id={"owners": peers[i], "sub": z}, device_id_type=MESH,
        )

    def flag_copy(i, source):
        return pltpu.make_async_remote_copy(
            src_ref=verdict.at[g], dst_ref=verdict.at[source],
            send_sem=flag_send.at[i], recv_sem=flag_recv.at[source],
            device_id={"groups": (g + i) % groups}, device_id_type=MESH,
        )

    pl.semaphore_wait(barrier, shards - 1 + groups - 1)
    for j in range(subs - 1):
        spare_copy(j).start()
    for j, i in pairs:
        news_copy(j, i, own).start()
    fill(0, base)
    for i in range(owners):
        row_copy(0, i, base).start()
    fill(subs - 1, cap)
    for i in range(owners - 1):
        row_copy(subs - 1, i, cap).start()
    own_copy = pltpu.make_async_copy(send.at[shards - 1], rows_ref.at[own], own_sem)
    own_copy.start()
    square = emb[...].astype(f32)
    square = square * square
    square_hi = square.astype(bf16)
    square_lo = (square - square_hi.astype(f32)).astype(bf16)
    ones = jnp.ones((8, width), bf16)
    total = lax.dot_general(ones, square_hi, CROSS, preferred_element_type=f32)
    total = total + lax.dot_general(ones, square_lo, CROSS, preferred_element_type=f32)
    inverse_row = lax.rsqrt(total[0:1] + 1e-06)
    table_copy.wait()
    given = jnp.zeros((1, rows), f32)
    others = jnp.full((1, rows), -1e30, f32)
    for lo in range(0, classes, 128):
        n = min(128, classes - lo)
        part = table[lo : lo + n, :]
        part_f = part.astype(f32)
        inverse_class = lax.rsqrt(jnp.sum(part_f * part_f, axis=1, keepdims=True) + 1e-06)
        scaled = lax.dot_general(part, emb[...], CROSS, preferred_element_type=f32) * inverse_class
        match = lax.broadcasted_iota(i32, (n, rows), 0) + lo == near
        given = given + jnp.sum(jnp.where(match, scaled, 0.0), axis=0, keepdims=True)
        others = jnp.maximum(others, jnp.max(jnp.where(match, -1e30, scaled), axis=0, keepdims=True))
    margin = (20.0 * (given * inverse_row - others * inverse_row)).astype(bf16).astype(f32)
    rank_hot = (lax.broadcasted_iota(i32, (wide, rows), 0) == rank).astype(f32).astype(bf16)
    marks = lax.dot_general((shard_hot * margin).astype(bf16), rank_hot, CROSS, preferred_element_type=f32)
    for t in range(shards):
        told[t] = marks[t : t + 1]
    scored[own] = told[own]
    fill(1, base)
    for j, i in pairs:
        score_copy(j, i, own).start()
    for j in range(1, subs - 1):
        if j > 1:
            fill(j, base)
        for i in range(owners):
            row_copy(j, i, base).start()
    order = [*range(1, subs - 1), 0]
    for j in order:
        spare_copy(j, True).wait_recv()
        for i in range(owners - 1):
            relay_copy(i, j, o).start()

    for j, i in pairs:
        news_copy(j, i, peers[i] * subs + planes[j]).wait_recv()
    for t in range(shards):
        heard_s[t : t + 1, :] = heard[t]
    counts = jnp.where(lax.broadcasted_iota(i32, (shards, wide), 1) >= lead, heard_s[...], 0.0)
    row_i, col_i = lax.broadcasted_iota(i32, (wide, wide), 0), lax.broadcasted_iota(i32, (wide, wide), 1)
    plane = ((row_i >= lead) & ((row_i - lead) % subs == col_i)).astype(f32)
    past = jnp.dot(jnp.maximum(counts - base, 0.0), plane, preferred_element_type=f32)
    away = lax.broadcasted_iota(i32, (shards, wide), 0) % subs != lax.broadcasted_iota(i32, (shards, wide), 1)
    most = jnp.max(jnp.max(jnp.where(away, past, 0.0), axis=1, keepdims=True), axis=0, keepdims=True)
    verdict[g] = jnp.broadcast_to(most, (1, wide))

    totals_ref[...] = jnp.sum(counts, axis=0, keepdims=True)[:, lead:].astype(i32)
    below = (
        lax.broadcasted_iota(i32, (shards, shards), 1) < lax.broadcasted_iota(i32, (shards, shards), 0)
    ).astype(f32)
    before = jnp.dot(below, counts, preferred_element_type=f32, precision=lax.Precision.HIGHEST)
    mine = lax.broadcasted_iota(i32, (shards, wide), 1) == own + lead
    count_col = jnp.sum(jnp.where(mine, counts, 0.0), axis=1, keepdims=True).astype(i32)
    before_col = jnp.sum(jnp.where(mine, before, 0.0), axis=1, keepdims=True).astype(i32)
    for i in range(1, groups):
        flag_copy(i, g).start()
    offset = lax.broadcasted_iota(i32, (shards, slots), 1) - cap * lax.broadcasted_iota(i32, (shards, slots), 0)
    inside = (offset >= 0) & (offset < cap)
    nook = jnp.sum(jnp.where(inside, offset, 0), axis=0, keepdims=True)
    filled = jnp.where(offset < count_col, before_col + offset, -1)
    position_ref[...] = jnp.sum(jnp.where(inside, filled, 0), axis=0, keepdims=True)

    def merge(a, j):
        s = a * subs + planes[j]
        nth_row = heard[s][:, base:cap].astype(i32)
        pick = (lax.broadcasted_iota(i32, (depth, cap - base), 0) + 1 == nth_row).astype(f32).astype(bf16)
        rest = lax.dot_general(pick, spill[a, ways[j] - 1], DOWN, preferred_element_type=f32)
        rows_ref[s, base:cap] = rest.astype(bf16)

    for j in order:
        merge(o, j)
    for i in range(1, groups):
        flag_copy(i, (g + groups - i) % groups).wait_recv()
    flag_ref[0] = (jnp.max(verdict[...]) > depth).astype(i32)
    for j in order:
        for i in range(owners - 1):
            relay_copy(i, j, peers[i]).wait_recv()
            merge(peers[i], j)

    for j, i in pairs:
        score_copy(j, i, peers[i] * subs + planes[j]).wait_recv()
    for t in range(shards):
        scores_s[t : t + 1, :] = scored[t]
    spread = (lax.broadcasted_iota(i32, (wide, slots), 0) == nook).astype(f32).astype(bf16)
    flat = jnp.dot(scores_s[...].astype(bf16), spread, preferred_element_type=f32)
    score_ref[...] = jnp.sum(jnp.where(inside, flat, 0.0), axis=0, keepdims=True).astype(score_ref.dtype)

    for i in range(1, groups):
        flag_copy(i, g).wait_send()
    for j in range(subs - 1):
        spare_copy(j).wait_send()
    for j in range(subs - 1):
        for i in range(owners - 1):
            relay_copy(i, j, o).wait_send()
    own_copy.wait()
    for j, i in pairs:
        news_copy(j, i, own).wait_send()
        score_copy(j, i, own).wait_send()
        row_copy(j, i, base if j < subs - 1 else cap).wait_send()
    for j, i in pairs:
        row_arrival(j, i, base if j < subs - 1 else cap).wait_recv()


def plain(call, embeddings, class_table, nearest, keep_class, destination):
    owners, subs = lax.axis_size("owners"), lax.axis_size("sub")
    shards = owners * subs
    rows, width = embeddings.shape
    classes = class_table.shape[0]
    cap = 3 * rows // (2 * shards)
    wide = up(max(shards, cap), 128)
    early = max(2, shards // 4)
    vmem = pl.BlockSpec(memory_space=pltpu.VMEM)
    hbm = pl.BlockSpec(memory_space=pl.ANY)
    f32, bf16, i32 = jnp.float32, jnp.bfloat16, jnp.int32
    dma = pltpu.SemaphoreType.DMA
    return pl.pallas_call(
        functools.partial(kernel, owners, subs, cap, early),
        out_shape=(
            pltpu.VMEM((shards, cap, width), bf16),
            pltpu.VMEM((1, shards * cap), f32),
            pltpu.VMEM((1, shards * cap), i32),
            pltpu.VMEM((1, wide), i32),
        ),
        in_specs=[hbm] * 5,
        out_specs=(vmem,) * 4,
        scratch_shapes=[
            pltpu.VMEM((1, rows), i32),
            pltpu.VMEM((1, classes), i32),
            pltpu.VMEM((1, rows), i32),
            pltpu.VMEM((rows, width), bf16),
            pltpu.VMEM((classes, width), bf16),
            pltpu.VMEM((up(up(classes, 128) // 128, 8), 128), f32),
            pltpu.VMEM((shards, cap, width), bf16),
            pltpu.VMEM((shards, 2, wide), f32),
            pltpu.VMEM((shards, 2, wide), f32),
            pltpu.VMEM((wide, wide), f32),
            pltpu.VMEM((shards, wide), f32),
            pltpu.VMEM((shards, wide), f32),
            pltpu.VMEM((1, rows), i32),
            dma((5,)),
            dma((shards,)),
            dma((shards,)),
            dma((shards,)),
            dma((shards,)),
            dma,
        ],
        compiler_params=pltpu.CompilerParams(collective_id=call, has_side_effects=True),
    )(
        nearest.reshape(1, rows),
        keep_class.reshape(1, classes),
        destination.reshape(1, rows),
        embeddings,
        class_table,
    )


def quick(base, depth, embeddings, class_table, nearest, keep_class, destination):
    groups, owners, subs = lax.axis_size("groups"), lax.axis_size("owners"), lax.axis_size("sub")
    shards = owners * subs
    rows, width = embeddings.shape
    classes = class_table.shape[0]
    cap = 3 * rows // (2 * shards)
    wide = up(shards + cap, 128)
    vmem = pl.BlockSpec(memory_space=pltpu.VMEM)
    hbm = pl.BlockSpec(memory_space=pl.ANY)
    f32, bf16, i32 = jnp.float32, jnp.bfloat16, jnp.int32
    dma = pltpu.SemaphoreType.DMA
    return pl.pallas_call(
        functools.partial(quick_kernel, groups, owners, subs, cap, base, depth),
        out_shape=(
            pltpu.VMEM((shards, cap, width), bf16),
            pltpu.VMEM((1, shards * cap), f32),
            pltpu.VMEM((1, shards * cap), i32),
            pltpu.VMEM((1, shards), i32),
            pltpu.SMEM((1,), i32),
        ),
        in_specs=[hbm] * 5,
        out_specs=(vmem,) * 4 + (pl.BlockSpec(memory_space=pltpu.SMEM),),
        scratch_shapes=[
            pltpu.VMEM((1, rows), i32),
            pltpu.VMEM((1, classes), i32),
            pltpu.VMEM((1, rows), i32),
            pltpu.VMEM((rows, width), bf16),
            pltpu.VMEM((classes, width), bf16),
            pltpu.VMEM((up(up(classes, 128) // 128, 8), 128), f32),
            pltpu.VMEM((rows, rows), bf16),
            pltpu.VMEM((shards, cap, width), bf16),
            pltpu.VMEM((subs - 1, depth, width), bf16),
            pltpu.VMEM((owners, subs - 1, depth, width), bf16),
            pltpu.VMEM((shards, 1, wide), f32),
            pltpu.VMEM((shards, 1, wide), f32),
            pltpu.VMEM((shards, 1, wide), f32),
            pltpu.VMEM((shards, 1, wide), f32),
            pltpu.VMEM((shards, wide), f32),
            pltpu.VMEM((shards, wide), f32),
            pltpu.VMEM((1, rows), i32),
            pltpu.VMEM((groups, 1, wide), f32),
            dma((5,)),
            dma((shards,)),
            dma((shards,)),
            dma((shards,)),
            dma((shards,)),
            dma((shards,)),
            dma((shards,)),
            dma((subs - 1,)),
            dma((subs - 1,)),
            dma((owners, subs - 1)),
            dma((owners, subs - 1)),
            dma((groups,)),
            dma((groups,)),
            dma,
        ],
        compiler_params=pltpu.CompilerParams(collective_id=0, has_side_effects=True),
    )(
        nearest.reshape(1, rows),
        keep_class.reshape(1, classes),
        destination.reshape(1, rows),
        embeddings,
        class_table,
    )


def close(got_rows, score, position, totals):
    shards, cap, width = got_rows.shape
    wide = totals.shape[1]
    vmem = pl.BlockSpec(memory_space=pltpu.VMEM)
    hbm = pl.BlockSpec(memory_space=pl.ANY)
    bf16, i32 = jnp.bfloat16, jnp.int32
    dma = pltpu.SemaphoreType.DMA
    small = [pltpu.with_memory_space_constraint(x, pltpu.VMEM) for x in (got_rows, score, position, totals)]
    rows_out, score_out, position_out, totals_out = pl.pallas_call(
        finish_kernel,
        out_shape=(
            jax.ShapeDtypeStruct((shards, cap, width), bf16),
            jax.ShapeDtypeStruct((shards * cap,), bf16),
            jax.ShapeDtypeStruct((shards * cap,), i32),
            jax.ShapeDtypeStruct((wide,), i32),
        ),
        in_specs=[vmem] * 4,
        out_specs=(hbm,) * 4,
        scratch_shapes=[
            pltpu.VMEM((shards * cap,), bf16),
            pltpu.VMEM((shards * cap,), i32),
            pltpu.VMEM((wide,), i32),
            dma((4,)),
        ],
    )(*small)
    return rows_out.reshape(shards * cap, width), score_out, position_out, totals_out[:shards]


def on_device(*args):
    rows = args[0].shape[0]
    subs, shards = lax.axis_size("sub"), lax.axis_size("owners") * lax.axis_size("sub")
    cap = 3 * rows // (2 * shards)
    base, depth = 2 * cap // 3, cap // 2
    if subs < 2 or shards % 8 or base % 16 or cap % 16 or depth % 8:
        return close(*plain(0, *args))
    *packed, flag = quick(base, depth, *args)

    def fast(inputs, results):
        return close(*results)

    def slow(inputs, results):
        return close(*plain(1, *inputs))

    return lax.cond(flag.reshape(()) > 0, slow, fast, args, tuple(packed))


def solution(mesh):
    in_specs = (
        P(("groups", "owners", "sub"), None),
        P(),
        P(("groups", "owners", "sub")),
        P(),
        P(("groups", "owners", "sub"), None),
    )
    out_specs = (
        P(("groups", "owners", "sub"), None),
        P(("groups", "owners", "sub")),
        P(("groups", "owners", "sub")),
        P("groups"),
    )
    return jax.shard_map(
        on_device, mesh=mesh, in_specs=in_specs, out_specs=out_specs, check_vma=False
    )
```

```python
import functools

import jax
import jax.numpy as jnp
from jax import lax
from jax.experimental import pallas as pl
from jax.experimental.pallas import tpu as pltpu
from jax.sharding import PartitionSpec as P

MESH = pl.DeviceIdType.MESH
CROSS = (((1,), (1,)), ((), ()))
DOWN = (((0,), (0,)), ((), ()))


def up(value, step):
    return (value + step - 1) // step * step


def place(owners, subs, k):
    o, z = lax.axis_index("owners"), lax.axis_index("sub")
    upper = (2 * z) // subs
    toward = upper * z + (1 - upper) * (subs - 1 - z)
    j = k // owners
    first = 1 - (j + subs - 1) // subs
    past = (j + subs - toward) // subs
    far = first * toward + (1 - first) * (j + past)
    to_sub = (z + far * (1 - 2 * upper) + subs) % subs
    to_owner = (o + 1 + k % owners) % owners
    return to_owner, to_sub


def finish_kernel(rows_ref, score_ref, position_ref, totals_ref, rows_out, score_out, position_out, totals_out,
                  score_s, position_s, totals_s, sem):
    copies = [pltpu.make_async_copy(rows_ref, rows_out, sem.at[0])]
    copies[0].start()
    position_s[...] = position_ref[...].reshape(position_s.shape)
    totals_s[...] = totals_ref[...].reshape(totals_s.shape)
    score_s[...] = score_ref[...].reshape(score_s.shape).astype(score_s.dtype)
    for i, (inner, outer) in enumerate(((position_s, position_out), (totals_s, totals_out), (score_s, score_out))):
        copies.append(pltpu.make_async_copy(inner, outer, sem.at[i + 1]))
        copies[-1].start()
    for copy in copies:
        copy.wait()


def kernel(owners, subs, cap, early, near_hbm, keep_hbm, dest_hbm, emb_hbm, table_hbm,
           rows_ref, score_ref, position_ref, totals_ref,
           near_ref, keep_ref, dest_ref, emb, table, keep2, send, meta, got, spots, counts_s, scores_s, slot_s,
           in_sem, send_sem, recv_sem, meta_send, meta_recv, own_sem):
    f32, bf16, i32 = jnp.float32, jnp.bfloat16, jnp.int32
    shards = owners * subs
    rows, width = emb.shape
    classes = table.shape[0]
    wide = meta.shape[2]
    slots = shards * cap
    o, z = lax.axis_index("owners"), lax.axis_index("sub")
    own = o * subs + z

    small = [
        pltpu.make_async_copy(near_hbm, near_ref, in_sem.at[2]),
        pltpu.make_async_copy(keep_hbm, keep_ref, in_sem.at[3]),
        pltpu.make_async_copy(dest_hbm, dest_ref, in_sem.at[4]),
    ]
    for copy in small:
        copy.start()
    emb_copy = pltpu.make_async_copy(emb_hbm, emb, in_sem.at[0])
    emb_copy.start()
    table_copy = pltpu.make_async_copy(table_hbm, table, in_sem.at[1])
    table_copy.start()

    barrier = pltpu.get_barrier_semaphore()

    def greet(k, c):
        a, b = place(owners, subs, k)
        pl.semaphore_signal(barrier, inc=1, device_id={"owners": a, "sub": b}, device_id_type=MESH)
        return c

    lax.fori_loop(0, shards - 1, greet, 0)

    for copy in small:
        copy.wait()
    near = near_ref[...]
    target = dest_ref[...]
    keep2[...] = jnp.zeros_like(keep2)
    for h in range(up(classes, 128) // 128):
        n = min(128, classes - h * 128)
        keep2[h : h + 1, :n] = keep_ref[:, h * 128 : h * 128 + n].astype(f32)
    deep = keep2.shape[0]
    high = near // 128
    low = near - high * 128
    low_hot = (lax.broadcasted_iota(i32, (128, rows), 0) == low).astype(f32).astype(bf16)
    by_high = jnp.dot(keep2[...].astype(bf16), low_hot, preferred_element_type=f32)
    kept = jnp.sum(
        jnp.where(lax.broadcasted_iota(i32, (deep, rows), 0) == high, by_high, 0.0), axis=0, keepdims=True
    )
    shard_hot = jnp.where(lax.broadcasted_iota(i32, (wide, rows), 0) == target, kept, 0.0)
    shard_bf = shard_hot.astype(bf16)
    earlier = (
        lax.broadcasted_iota(i32, (rows, rows), 0) < lax.broadcasted_iota(i32, (rows, rows), 1)
    ).astype(f32).astype(bf16)
    running = jnp.dot(shard_bf, earlier, preferred_element_type=f32)
    rank = jnp.sum(shard_hot * running, axis=0, keepdims=True).astype(i32)
    slot_s[...] = jnp.where(kept > 0.5, target * cap + rank, -1)

    emb_copy.wait()

    def fill(k):
        a, b = place(owners, subs, k)
        t = a * subs + b
        hot = (slot_s[...] == t * cap + lax.broadcasted_iota(i32, (cap, rows), 0)).astype(f32).astype(bf16)
        send[k] = jnp.dot(hot, emb[...], preferred_element_type=f32).astype(bf16)

    def row_copy(k, source):
        a, b = place(owners, subs, k)
        return pltpu.make_async_remote_copy(
            src_ref=send.at[k], dst_ref=rows_ref.at[source],
            send_sem=send_sem.at[k], recv_sem=recv_sem.at[source],
            device_id={"owners": a, "sub": b}, device_id_type=MESH,
        )

    def meta_copy(k, source):
        a, b = place(owners, subs, k)
        return pltpu.make_async_remote_copy(
            src_ref=meta.at[k], dst_ref=got.at[source],
            send_sem=meta_send.at[k], recv_sem=meta_recv.at[source],
            device_id={"owners": a, "sub": b}, device_id_type=MESH,
        )

    def step(k, c):
        fill(k)
        row_copy(k - 1, own).start()
        return c

    fill(0)
    fill(1)
    pl.semaphore_wait(barrier, shards - 1)
    row_copy(0, own).start()
    lax.fori_loop(2, early, step, 0)

    square = emb[...].astype(f32)
    square = square * square
    square_hi = square.astype(bf16)
    square_lo = (square - square_hi.astype(f32)).astype(bf16)
    ones = jnp.ones((8, width), bf16)
    total = lax.dot_general(ones, square_hi, CROSS, preferred_element_type=f32)
    total = total + lax.dot_general(ones, square_lo, CROSS, preferred_element_type=f32)
    inverse_row = lax.rsqrt(total[0:1] + 1e-06)
    table_copy.wait()
    given = jnp.zeros((1, rows), f32)
    others = jnp.full((1, rows), -1e30, f32)
    for lo in range(0, classes, 128):
        n = min(128, classes - lo)
        part = table[lo : lo + n, :]
        part_f = part.astype(f32)
        inverse_class = lax.rsqrt(jnp.sum(part_f * part_f, axis=1, keepdims=True) + 1e-06)
        scaled = lax.dot_general(part, emb[...], CROSS, preferred_element_type=f32) * inverse_class
        match = lax.broadcasted_iota(i32, (n, rows), 0) + lo == near
        given = given + jnp.sum(jnp.where(match, scaled, 0.0), axis=0, keepdims=True)
        others = jnp.maximum(others, jnp.max(jnp.where(match, -1e30, scaled), axis=0, keepdims=True))
    margin = (20.0 * (given * inverse_row - others * inverse_row)).astype(bf16).astype(f32)
    rank_hot = (lax.broadcasted_iota(i32, (spots.shape[1], rows), 0) == rank).astype(f32).astype(bf16)
    spots[...] = lax.dot_general((shard_hot * margin).astype(bf16), rank_hot, CROSS, preferred_element_type=f32)
    counts = lax.dot_general(jnp.ones((8, rows), bf16), shard_bf, CROSS, preferred_element_type=f32)[0:1]

    def fill_meta(k, c):
        a, b = place(owners, subs, k)
        meta[k, 0:1, :] = spots[pl.ds(a * subs + b, 1), :]
        meta[k, 1:2, :] = counts
        return c

    lax.fori_loop(0, shards - 1, fill_meta, 0)
    got[own, 0:1, :] = spots[pl.ds(own, 1), :]
    got[own, 1:2, :] = counts

    lax.fori_loop(early, early + 1, step, 0)

    def send_meta(k, c):
        meta_copy(k, own).start()
        return c

    lax.fori_loop(0, shards - 1, send_meta, 0)
    lax.fori_loop(early + 1, shards, step, 0)
    own_copy = pltpu.make_async_copy(send.at[shards - 1], rows_ref.at[own], own_sem)
    own_copy.start()

    def take_meta(k, c):
        source = (own + 1 + k) % shards
        meta_copy(k, source).wait_recv()
        return c

    lax.fori_loop(0, shards - 1, take_meta, 0)

    def lay(s, c):
        scores_s[pl.ds(s, 1), :] = got[s, 0:1, :]
        counts_s[pl.ds(s, 1), :] = got[s, 1:2, :]
        return c

    lax.fori_loop(0, shards, lay, 0)
    table_counts = counts_s[...]
    totals_ref[...] = jnp.sum(table_counts, axis=0, keepdims=True).astype(i32)
    below = (
        lax.broadcasted_iota(i32, (shards, shards), 1) < lax.broadcasted_iota(i32, (shards, shards), 0)
    ).astype(f32)
    before = jnp.dot(below, table_counts, preferred_element_type=f32, precision=lax.Precision.HIGHEST)
    mine = lax.broadcasted_iota(i32, (shards, wide), 1) == own
    count_col = jnp.sum(jnp.where(mine, table_counts, 0.0), axis=1, keepdims=True).astype(i32)
    before_col = jnp.sum(jnp.where(mine, before, 0.0), axis=1, keepdims=True).astype(i32)
    offset = lax.broadcasted_iota(i32, (shards, slots), 1) - cap * lax.broadcasted_iota(i32, (shards, slots), 0)
    inside = (offset >= 0) & (offset < cap)
    spot = jnp.sum(jnp.where(inside, offset, 0), axis=0, keepdims=True)
    filled = jnp.where(offset < count_col, before_col + offset, -1)
    position_ref[...] = jnp.sum(jnp.where(inside, filled, 0), axis=0, keepdims=True)
    spread = (lax.broadcasted_iota(i32, (wide, slots), 0) == spot).astype(f32).astype(bf16)
    flat = jnp.dot(scores_s[...].astype(bf16), spread, preferred_element_type=f32)
    score_ref[...] = jnp.sum(jnp.where(inside, flat, 0.0), axis=0, keepdims=True).astype(score_ref.dtype)

    def finish(k, c):
        source = (own + 1 + k) % shards
        row_copy(k, source).wait_recv()
        row_copy(k, own).wait_send()
        meta_copy(k, own).wait_send()
        return c

    lax.fori_loop(0, shards - 1, finish, 0)
    own_copy.wait()


def quick_kernel(groups, owners, subs, cap, base, depth, near_hbm, keep_hbm, dest_hbm, emb_hbm, table_hbm,
                 rows_ref, score_ref, position_ref, totals_ref, flag_ref,
                 near_ref, keep_ref, dest_ref, emb, table, keep2, earlier, send, spare, spill, news, heard, told, scored,
                 heard_s, scores_s, slot_s, verdict,
                 in_sem, send_sem, recv_sem, news_send, news_recv, score_send, score_recv, spare_send, spare_recv,
                 relay_send, relay_recv, flag_send, flag_recv, own_sem, mutual):
    f32, bf16, i32 = jnp.float32, jnp.bfloat16, jnp.int32
    shards = owners * subs
    rows, width = emb.shape
    classes = table.shape[0]
    wide = news.shape[2]
    lead = wide - shards
    slots = shards * cap
    g, o, z = lax.axis_index("groups"), lax.axis_index("owners"), lax.axis_index("sub")
    own = o * subs + z
    peers = [(o + 1 + i) % owners for i in range(owners)]
    planes = [place(owners, subs, j * owners)[1] for j in range(subs)]

    small = [
        pltpu.make_async_copy(near_hbm, near_ref, in_sem.at[2]),
        pltpu.make_async_copy(keep_hbm, keep_ref, in_sem.at[3]),
        pltpu.make_async_copy(dest_hbm, dest_ref, in_sem.at[4]),
    ]
    for copy in small:
        copy.start()
    emb_copy = pltpu.make_async_copy(emb_hbm, emb, in_sem.at[0])
    emb_copy.start()
    table_copy = pltpu.make_async_copy(table_hbm, table, in_sem.at[1])
    table_copy.start()

    def device(j, i):
        return {"owners": peers[i], "sub": planes[j]}

    pairs = [(j, i) for j in range(subs) for i in range(owners)][: shards - 1]
    half = subs // 2
    upper = (2 * z) // subs
    cross = [(1 - upper) * (subs - 1 - m) + upper * m for m in range(half)]
    mates = [upper * half + (z - upper * half + m) % half for m in range(1, half)]
    barrier = pltpu.get_barrier_semaphore()
    for b in cross:
        for a in peers:
            pl.semaphore_signal(barrier, inc=1, device_id={"owners": a, "sub": b}, device_id_type=MESH)
    for i in range(1, groups):
        pl.semaphore_signal(barrier, inc=1, device_id={"groups": (g + i) % groups}, device_id_type=MESH)

    earlier[...] = (
        lax.broadcasted_iota(i32, (rows, rows), 0) < lax.broadcasted_iota(i32, (rows, rows), 1)
    ).astype(f32).astype(bf16)
    keep2[...] = jnp.zeros_like(keep2)
    for copy in small:
        copy.wait()
    near = near_ref[...]
    target = dest_ref[...]
    for h in range(up(classes, 128) // 128):
        n = min(128, classes - h * 128)
        keep2[h : h + 1, :n] = keep_ref[:, h * 128 : h * 128 + n].astype(f32)
    deep = keep2.shape[0]
    high = near // 128
    low = near - high * 128
    low_hot = (lax.broadcasted_iota(i32, (128, rows), 0) == low).astype(f32).astype(bf16)
    by_high = jnp.dot(keep2[...].astype(bf16), low_hot, preferred_element_type=f32)
    kept = jnp.sum(
        jnp.where(lax.broadcasted_iota(i32, (deep, rows), 0) == high, by_high, 0.0), axis=0, keepdims=True
    )
    shard_hot = jnp.where(lax.broadcasted_iota(i32, (up(shards, 8), rows), 0) == target, kept, 0.0)
    running = jnp.dot(shard_hot.astype(bf16), earlier[...], preferred_element_type=f32)
    rank = jnp.sum(shard_hot * running, axis=0, keepdims=True).astype(i32)
    slot_s[...] = jnp.where(kept > 0.5, target * cap + rank, -1)

    ahead = target - target // subs * subs - z
    ahead = jnp.where(ahead < 0, ahead + subs, ahead)
    over = (kept > 0.5) & (rank >= base) & (ahead > 0)
    plane_hot = jnp.where((lax.broadcasted_iota(i32, (up(subs, 8), rows), 0) == ahead) & over, 1.0, 0.0)
    before_it = jnp.dot(plane_hot.astype(bf16), earlier[...], preferred_element_type=f32)
    spot = jnp.sum(plane_hot * before_it, axis=0, keepdims=True).astype(i32)
    fits = over & (spot < depth)
    nth = jnp.where(fits, spot + 1, 0).astype(f32)

    rank_hot = (lax.broadcasted_iota(i32, (wide, rows), 0) == rank).astype(f32).astype(bf16)
    count_hot = jnp.where(lax.broadcasted_iota(i32, (wide, rows), 0) == target + lead, kept, 0.0).astype(bf16)
    notes = lax.dot_general((shard_hot * nth).astype(bf16), rank_hot, CROSS, preferred_element_type=f32)
    notes = notes + lax.dot_general(
        jnp.ones((up(shards, 8), rows), bf16), count_hot, CROSS, preferred_element_type=f32
    )
    for t in range(shards):
        news[t] = notes[t : t + 1]
    heard[own] = news[own]

    emb_copy.wait()

    seat = jnp.where(fits, (ahead - 1) * depth + spot, -1)
    hot = (lax.broadcasted_iota(i32, ((subs - 1) * depth, rows), 0) == seat).astype(f32).astype(bf16)
    packed = jnp.dot(hot, emb[...], preferred_element_type=f32).astype(bf16)
    for d in range(subs - 1):
        spare[d] = packed[d * depth : (d + 1) * depth]

    def fill(j, n):
        slot = slot_s[...] - planes[j] * cap
        hot = jnp.concatenate([
            (slot - a * subs * cap == lax.broadcasted_iota(i32, (n, rows), 0)).astype(f32).astype(bf16) for a in peers
        ])
        block = jnp.dot(hot, emb[...], preferred_element_type=f32).astype(bf16)
        for i in range(owners):
            send[j * owners + i, :n] = block[i * n : (i + 1) * n]

    def row_copy(j, i, n):
        k = j * owners + i
        return pltpu.make_async_remote_copy(
            src_ref=send.at[k, :n], dst_ref=rows_ref.at[own, :n],
            send_sem=send_sem.at[k], recv_sem=recv_sem.at[own],
            device_id=device(j, i), device_id_type=MESH,
        )

    def row_arrival(j, i, n):
        source = peers[i] * subs + planes[j]
        return pltpu.make_async_remote_copy(
            src_ref=send.at[0, :n], dst_ref=rows_ref.at[source, :n],
            send_sem=send_sem.at[0], recv_sem=recv_sem.at[source],
            device_id=device(j, i), device_id_type=MESH,
        )

    def note_copy(a, b, ref, landing, out_sem, in_sem, source):
        t = a * subs + b
        return pltpu.make_async_remote_copy(
            src_ref=ref.at[t], dst_ref=landing.at[source],
            send_sem=out_sem.at[t], recv_sem=in_sem.at[source],
            device_id={"owners": a, "sub": b}, device_id_type=MESH,
        )

    def news_copy(a, b, source):
        return note_copy(a, b, news, heard, news_send, news_recv, source)

    def score_copy(j, i, source):
        return note_copy(peers[i], planes[j], told, scored, score_send, score_recv, source)

    ways = [(b - z + subs) % subs for b in planes[: subs - 1]]

    def spare_copy(b, arrival=False):
        way = (b - z + subs) % subs
        slot = way - 1 if arrival else subs - 1 - way
        return pltpu.make_async_remote_copy(
            src_ref=spare.at[way - 1], dst_ref=spill.at[o, slot],
            send_sem=spare_send.at[way - 1], recv_sem=spare_recv.at[slot],
            device_id={"owners": o, "sub": b}, device_id_type=MESH,
        )

    def relay_copy(i, j, source):
        slot = ways[j] - 1
        return pltpu.make_async_remote_copy(
            src_ref=spill.at[source, slot], dst_ref=spill.at[source, slot],
            send_sem=relay_send.at[i, slot], recv_sem=relay_recv.at[source, slot],
            device_id={"owners": peers[i], "sub": z}, device_id_type=MESH,
        )

    def flag_copy(i, source):
        return pltpu.make_async_remote_copy(
            src_ref=verdict.at[g], dst_ref=verdict.at[source],
            send_sem=flag_send.at[i], recv_sem=flag_recv.at[source],
            device_id={"groups": (g + i) % groups}, device_id_type=MESH,
        )

    pl.semaphore_wait(barrier, half * owners + groups - 1)
    pl.semaphore_signal(
        mutual, inc=1, device_id={"owners": o, "sub": (z + half) % subs}, device_id_type=MESH
    )
    for b in cross:
        spare_copy(b).start()
    for b in cross:
        for a in peers:
            news_copy(a, b, own).start()
    fill(0, base)
    for i in range(owners):
        row_copy(0, i, base).start()
    fill(subs - 1, cap)
    pl.semaphore_wait(mutual, 1)
    for b in mates:
        spare_copy(b).start()
    for b in [*mates, z]:
        for a in peers[: owners - 1] if b is z else peers:
            news_copy(a, b, own).start()
    for i in range(owners - 1):
        row_copy(subs - 1, i, cap).start()
    own_copy = pltpu.make_async_copy(send.at[shards - 1], rows_ref.at[own], own_sem)
    own_copy.start()
    square = emb[...].astype(f32)
    square = square * square
    square_hi = square.astype(bf16)
    square_lo = (square - square_hi.astype(f32)).astype(bf16)
    ones = jnp.ones((8, width), bf16)
    total = lax.dot_general(ones, square_hi, CROSS, preferred_element_type=f32)
    total = total + lax.dot_general(ones, square_lo, CROSS, preferred_element_type=f32)
    inverse_row = lax.rsqrt(total[0:1] + 1e-06)
    table_copy.wait()
    given = jnp.zeros((1, rows), f32)
    others = jnp.full((1, rows), -1e30, f32)
    for lo in range(0, classes, 128):
        n = min(128, classes - lo)
        part = table[lo : lo + n, :]
        part_f = part.astype(f32)
        inverse_class = lax.rsqrt(jnp.sum(part_f * part_f, axis=1, keepdims=True) + 1e-06)
        scaled = lax.dot_general(part, emb[...], CROSS, preferred_element_type=f32) * inverse_class
        match = lax.broadcasted_iota(i32, (n, rows), 0) + lo == near
        given = given + jnp.sum(jnp.where(match, scaled, 0.0), axis=0, keepdims=True)
        others = jnp.maximum(others, jnp.max(jnp.where(match, -1e30, scaled), axis=0, keepdims=True))
    margin = (20.0 * (given * inverse_row - others * inverse_row)).astype(bf16).astype(f32)
    rank_hot = (lax.broadcasted_iota(i32, (wide, rows), 0) == rank).astype(f32).astype(bf16)
    marks = lax.dot_general((shard_hot * margin).astype(bf16), rank_hot, CROSS, preferred_element_type=f32)
    for t in range(shards):
        told[t] = marks[t : t + 1]
    scored[own] = told[own]
    fill(1, base)
    for j, i in pairs:
        score_copy(j, i, own).start()
    for j in range(1, subs - 1):
        if j > 1:
            fill(j, base)
        for i in range(owners):
            row_copy(j, i, base).start()
    order = [*range(1, subs - 1), 0]
    for j in order:
        spare_copy(planes[j], True).wait_recv()
        for i in range(owners - 1):
            relay_copy(i, j, o).start()

    for j, i in pairs:
        news_copy(peers[i], planes[j], peers[i] * subs + planes[j]).wait_recv()
    for t in range(shards):
        heard_s[t : t + 1, :] = heard[t]
    counts = jnp.where(lax.broadcasted_iota(i32, (shards, wide), 1) >= lead, heard_s[...], 0.0)
    row_i, col_i = lax.broadcasted_iota(i32, (wide, wide), 0), lax.broadcasted_iota(i32, (wide, wide), 1)
    plane = ((row_i >= lead) & ((row_i - lead) % subs == col_i)).astype(f32)
    past = jnp.dot(jnp.maximum(counts - base, 0.0), plane, preferred_element_type=f32)
    away = lax.broadcasted_iota(i32, (shards, wide), 0) % subs != lax.broadcasted_iota(i32, (shards, wide), 1)
    most = jnp.max(jnp.max(jnp.where(away, past, 0.0), axis=1, keepdims=True), axis=0, keepdims=True)
    verdict[g] = jnp.broadcast_to(most, (1, wide))

    totals_ref[...] = jnp.sum(counts, axis=0, keepdims=True)[:, lead:].astype(i32)
    below = (
        lax.broadcasted_iota(i32, (shards, shards), 1) < lax.broadcasted_iota(i32, (shards, shards), 0)
    ).astype(f32)
    before = jnp.dot(below, counts, preferred_element_type=f32, precision=lax.Precision.HIGHEST)
    mine = lax.broadcasted_iota(i32, (shards, wide), 1) == own + lead
    count_col = jnp.sum(jnp.where(mine, counts, 0.0), axis=1, keepdims=True).astype(i32)
    before_col = jnp.sum(jnp.where(mine, before, 0.0), axis=1, keepdims=True).astype(i32)
    for i in range(1, groups):
        flag_copy(i, g).start()
    offset = lax.broadcasted_iota(i32, (shards, slots), 1) - cap * lax.broadcasted_iota(i32, (shards, slots), 0)
    inside = (offset >= 0) & (offset < cap)
    nook = jnp.sum(jnp.where(inside, offset, 0), axis=0, keepdims=True)
    filled = jnp.where(offset < count_col, before_col + offset, -1)
    position_ref[...] = jnp.sum(jnp.where(inside, filled, 0), axis=0, keepdims=True)

    def merge(a, j):
        s = a * subs + planes[j]
        nth_row = heard[s][:, base:cap].astype(i32)
        pick = (lax.broadcasted_iota(i32, (depth, cap - base), 0) + 1 == nth_row).astype(f32).astype(bf16)
        rest = lax.dot_general(pick, spill[a, ways[j] - 1], DOWN, preferred_element_type=f32)
        rows_ref[s, base:cap] = rest.astype(bf16)

    for j in order:
        merge(o, j)
    for i in range(1, groups):
        flag_copy(i, (g + groups - i) % groups).wait_recv()
    flag_ref[0] = (jnp.max(verdict[...]) > depth).astype(i32)
    for j in order:
        for i in range(owners - 1):
            relay_copy(i, j, peers[i]).wait_recv()
            merge(peers[i], j)

    for j, i in pairs:
        score_copy(j, i, peers[i] * subs + planes[j]).wait_recv()
    for t in range(shards):
        scores_s[t : t + 1, :] = scored[t]
    spread = (lax.broadcasted_iota(i32, (wide, slots), 0) == nook).astype(f32).astype(bf16)
    flat = jnp.dot(scores_s[...].astype(bf16), spread, preferred_element_type=f32)
    score_ref[...] = jnp.sum(jnp.where(inside, flat, 0.0), axis=0, keepdims=True).astype(score_ref.dtype)

    for i in range(1, groups):
        flag_copy(i, g).wait_send()
    for j in range(subs - 1):
        spare_copy(planes[j]).wait_send()
    for j in range(subs - 1):
        for i in range(owners - 1):
            relay_copy(i, j, o).wait_send()
    own_copy.wait()
    for j, i in pairs:
        news_copy(peers[i], planes[j], own).wait_send()
        score_copy(j, i, own).wait_send()
        row_copy(j, i, base if j < subs - 1 else cap).wait_send()
    for j, i in pairs:
        row_arrival(j, i, base if j < subs - 1 else cap).wait_recv()


def plain(call, embeddings, class_table, nearest, keep_class, destination):
    owners, subs = lax.axis_size("owners"), lax.axis_size("sub")
    shards = owners * subs
    rows, width = embeddings.shape
    classes = class_table.shape[0]
    cap = 3 * rows // (2 * shards)
    wide = up(max(shards, cap), 128)
    early = max(2, shards // 4)
    vmem = pl.BlockSpec(memory_space=pltpu.VMEM)
    hbm = pl.BlockSpec(memory_space=pl.ANY)
    f32, bf16, i32 = jnp.float32, jnp.bfloat16, jnp.int32
    dma = pltpu.SemaphoreType.DMA
    return pl.pallas_call(
        functools.partial(kernel, owners, subs, cap, early),
        out_shape=(
            pltpu.VMEM((shards, cap, width), bf16),
            pltpu.VMEM((1, shards * cap), f32),
            pltpu.VMEM((1, shards * cap), i32),
            pltpu.VMEM((1, wide), i32),
        ),
        in_specs=[hbm] * 5,
        out_specs=(vmem,) * 4,
        scratch_shapes=[
            pltpu.VMEM((1, rows), i32),
            pltpu.VMEM((1, classes), i32),
            pltpu.VMEM((1, rows), i32),
            pltpu.VMEM((rows, width), bf16),
            pltpu.VMEM((classes, width), bf16),
            pltpu.VMEM((up(up(classes, 128) // 128, 8), 128), f32),
            pltpu.VMEM((shards, cap, width), bf16),
            pltpu.VMEM((shards, 2, wide), f32),
            pltpu.VMEM((shards, 2, wide), f32),
            pltpu.VMEM((wide, wide), f32),
            pltpu.VMEM((shards, wide), f32),
            pltpu.VMEM((shards, wide), f32),
            pltpu.VMEM((1, rows), i32),
            dma((5,)),
            dma((shards,)),
            dma((shards,)),
            dma((shards,)),
            dma((shards,)),
            dma,
        ],
        compiler_params=pltpu.CompilerParams(collective_id=call, has_side_effects=True),
    )(
        nearest.reshape(1, rows),
        keep_class.reshape(1, classes),
        destination.reshape(1, rows),
        embeddings,
        class_table,
    )


def quick(base, depth, embeddings, class_table, nearest, keep_class, destination):
    groups, owners, subs = lax.axis_size("groups"), lax.axis_size("owners"), lax.axis_size("sub")
    shards = owners * subs
    rows, width = embeddings.shape
    classes = class_table.shape[0]
    cap = 3 * rows // (2 * shards)
    wide = up(shards + cap, 128)
    vmem = pl.BlockSpec(memory_space=pltpu.VMEM)
    hbm = pl.BlockSpec(memory_space=pl.ANY)
    f32, bf16, i32 = jnp.float32, jnp.bfloat16, jnp.int32
    dma = pltpu.SemaphoreType.DMA
    return pl.pallas_call(
        functools.partial(quick_kernel, groups, owners, subs, cap, base, depth),
        out_shape=(
            pltpu.VMEM((shards, cap, width), bf16),
            pltpu.VMEM((1, shards * cap), f32),
            pltpu.VMEM((1, shards * cap), i32),
            pltpu.VMEM((1, shards), i32),
            pltpu.SMEM((1,), i32),
        ),
        in_specs=[hbm] * 5,
        out_specs=(vmem,) * 4 + (pl.BlockSpec(memory_space=pltpu.SMEM),),
        scratch_shapes=[
            pltpu.VMEM((1, rows), i32),
            pltpu.VMEM((1, classes), i32),
            pltpu.VMEM((1, rows), i32),
            pltpu.VMEM((rows, width), bf16),
            pltpu.VMEM((classes, width), bf16),
            pltpu.VMEM((up(up(classes, 128) // 128, 8), 128), f32),
            pltpu.VMEM((rows, rows), bf16),
            pltpu.VMEM((shards, cap, width), bf16),
            pltpu.VMEM((subs - 1, depth, width), bf16),
            pltpu.VMEM((owners, subs - 1, depth, width), bf16),
            pltpu.VMEM((shards, 1, wide), f32),
            pltpu.VMEM((shards, 1, wide), f32),
            pltpu.VMEM((shards, 1, wide), f32),
            pltpu.VMEM((shards, 1, wide), f32),
            pltpu.VMEM((shards, wide), f32),
            pltpu.VMEM((shards, wide), f32),
            pltpu.VMEM((1, rows), i32),
            pltpu.VMEM((groups, 1, wide), f32),
            dma((5,)),
            dma((shards,)),
            dma((shards,)),
            dma((shards,)),
            dma((shards,)),
            dma((shards,)),
            dma((shards,)),
            dma((subs - 1,)),
            dma((subs - 1,)),
            dma((owners, subs - 1)),
            dma((owners, subs - 1)),
            dma((groups,)),
            dma((groups,)),
            dma,
            pltpu.SemaphoreType.REGULAR,
        ],
        compiler_params=pltpu.CompilerParams(collective_id=0, has_side_effects=True),
    )(
        nearest.reshape(1, rows),
        keep_class.reshape(1, classes),
        destination.reshape(1, rows),
        embeddings,
        class_table,
    )


def close(got_rows, score, position, totals):
    shards, cap, width = got_rows.shape
    wide = totals.shape[1]
    vmem = pl.BlockSpec(memory_space=pltpu.VMEM)
    hbm = pl.BlockSpec(memory_space=pl.ANY)
    bf16, i32 = jnp.bfloat16, jnp.int32
    dma = pltpu.SemaphoreType.DMA
    small = [pltpu.with_memory_space_constraint(x, pltpu.VMEM) for x in (got_rows, score, position, totals)]
    rows_out, score_out, position_out, totals_out = pl.pallas_call(
        finish_kernel,
        out_shape=(
            jax.ShapeDtypeStruct((shards, cap, width), bf16),
            jax.ShapeDtypeStruct((shards * cap,), bf16),
            jax.ShapeDtypeStruct((shards * cap,), i32),
            jax.ShapeDtypeStruct((wide,), i32),
        ),
        in_specs=[vmem] * 4,
        out_specs=(hbm,) * 4,
        scratch_shapes=[
            pltpu.VMEM((shards * cap,), bf16),
            pltpu.VMEM((shards * cap,), i32),
            pltpu.VMEM((wide,), i32),
            dma((4,)),
        ],
    )(*small)
    return rows_out.reshape(shards * cap, width), score_out, position_out, totals_out[:shards]


def on_device(*args):
    rows = args[0].shape[0]
    subs, shards = lax.axis_size("sub"), lax.axis_size("owners") * lax.axis_size("sub")
    cap = 3 * rows // (2 * shards)
    base, depth = 2 * cap // 3, cap // 2
    if subs % 2 or shards % 8 or base % 16 or cap % 16 or depth % 8:
        return close(*plain(0, *args))
    *packed, flag = quick(base, depth, *args)

    def fast(inputs, results):
        return close(*results)

    def slow(inputs, results):
        return close(*plain(1, *inputs))

    return lax.cond(flag.reshape(()) > 0, slow, fast, args, tuple(packed))


def solution(mesh):
    in_specs = (
        P(("groups", "owners", "sub"), None),
        P(),
        P(("groups", "owners", "sub")),
        P(),
        P(("groups", "owners", "sub"), None),
    )
    out_specs = (
        P(("groups", "owners", "sub"), None),
        P(("groups", "owners", "sub")),
        P(("groups", "owners", "sub")),
        P("groups"),
    )
    return jax.shard_map(
        on_device, mesh=mesh, in_specs=in_specs, out_specs=out_specs, check_vma=False
    )
```

```python
import functools

import jax
import jax.numpy as jnp
from jax import lax
from jax.experimental import pallas as pl
from jax.experimental.pallas import tpu as pltpu
from jax.sharding import PartitionSpec as P

MESH = pl.DeviceIdType.MESH
CROSS = (((1,), (1,)), ((), ()))
DOWN = (((0,), (0,)), ((), ()))


def up(value, step):
    return (value + step - 1) // step * step


def place(owners, subs, k):
    o, z = lax.axis_index("owners"), lax.axis_index("sub")
    upper = (2 * z) // subs
    toward = upper * z + (1 - upper) * (subs - 1 - z)
    j = k // owners
    first = 1 - (j + subs - 1) // subs
    past = (j + subs - toward) // subs
    far = first * toward + (1 - first) * (j + past)
    to_sub = (z + far * (1 - 2 * upper) + subs) % subs
    to_owner = (o + 1 + k % owners) % owners
    return to_owner, to_sub


def finish_kernel(rows_ref, score_ref, position_ref, totals_ref, rows_out, score_out, position_out, totals_out,
                  score_s, position_s, totals_s, sem):
    copies = [pltpu.make_async_copy(rows_ref, rows_out, sem.at[0])]
    copies[0].start()
    position_s[...] = position_ref[...].reshape(position_s.shape)
    totals_s[...] = totals_ref[...].reshape(totals_s.shape)
    score_s[...] = score_ref[...].reshape(score_s.shape).astype(score_s.dtype)
    for i, (inner, outer) in enumerate(((position_s, position_out), (totals_s, totals_out), (score_s, score_out))):
        copies.append(pltpu.make_async_copy(inner, outer, sem.at[i + 1]))
        copies[-1].start()
    for copy in copies:
        copy.wait()


def kernel(owners, subs, cap, early, near_hbm, keep_hbm, dest_hbm, emb_hbm, table_hbm,
           rows_ref, score_ref, position_ref, totals_ref,
           near_ref, keep_ref, dest_ref, emb, table, keep2, send, meta, got, spots, counts_s, scores_s, slot_s,
           in_sem, send_sem, recv_sem, meta_send, meta_recv, own_sem):
    f32, bf16, i32 = jnp.float32, jnp.bfloat16, jnp.int32
    shards = owners * subs
    rows, width = emb.shape
    classes = table.shape[0]
    wide = meta.shape[2]
    slots = shards * cap
    o, z = lax.axis_index("owners"), lax.axis_index("sub")
    own = o * subs + z

    small = [
        pltpu.make_async_copy(near_hbm, near_ref, in_sem.at[2]),
        pltpu.make_async_copy(keep_hbm, keep_ref, in_sem.at[3]),
        pltpu.make_async_copy(dest_hbm, dest_ref, in_sem.at[4]),
    ]
    for copy in small:
        copy.start()
    emb_copy = pltpu.make_async_copy(emb_hbm, emb, in_sem.at[0])
    emb_copy.start()
    table_copy = pltpu.make_async_copy(table_hbm, table, in_sem.at[1])
    table_copy.start()

    barrier = pltpu.get_barrier_semaphore()

    def greet(k, c):
        a, b = place(owners, subs, k)
        pl.semaphore_signal(barrier, inc=1, device_id={"owners": a, "sub": b}, device_id_type=MESH)
        return c

    lax.fori_loop(0, shards - 1, greet, 0)

    for copy in small:
        copy.wait()
    near = near_ref[...]
    target = dest_ref[...]
    keep2[...] = jnp.zeros_like(keep2)
    for h in range(up(classes, 128) // 128):
        n = min(128, classes - h * 128)
        keep2[h : h + 1, :n] = keep_ref[:, h * 128 : h * 128 + n].astype(f32)
    deep = keep2.shape[0]
    high = near // 128
    low = near - high * 128
    low_hot = (lax.broadcasted_iota(i32, (128, rows), 0) == low).astype(f32).astype(bf16)
    by_high = jnp.dot(keep2[...].astype(bf16), low_hot, preferred_element_type=f32)
    kept = jnp.sum(
        jnp.where(lax.broadcasted_iota(i32, (deep, rows), 0) == high, by_high, 0.0), axis=0, keepdims=True
    )
    shard_hot = jnp.where(lax.broadcasted_iota(i32, (wide, rows), 0) == target, kept, 0.0)
    shard_bf = shard_hot.astype(bf16)
    earlier = (
        lax.broadcasted_iota(i32, (rows, rows), 0) < lax.broadcasted_iota(i32, (rows, rows), 1)
    ).astype(f32).astype(bf16)
    running = jnp.dot(shard_bf, earlier, preferred_element_type=f32)
    rank = jnp.sum(shard_hot * running, axis=0, keepdims=True).astype(i32)
    slot_s[...] = jnp.where(kept > 0.5, target * cap + rank, -1)

    emb_copy.wait()

    def fill(k):
        a, b = place(owners, subs, k)
        t = a * subs + b
        hot = (slot_s[...] == t * cap + lax.broadcasted_iota(i32, (cap, rows), 0)).astype(f32).astype(bf16)
        send[k] = jnp.dot(hot, emb[...], preferred_element_type=f32).astype(bf16)

    def row_copy(k, source):
        a, b = place(owners, subs, k)
        return pltpu.make_async_remote_copy(
            src_ref=send.at[k], dst_ref=rows_ref.at[source],
            send_sem=send_sem.at[k], recv_sem=recv_sem.at[source],
            device_id={"owners": a, "sub": b}, device_id_type=MESH,
        )

    def meta_copy(k, source):
        a, b = place(owners, subs, k)
        return pltpu.make_async_remote_copy(
            src_ref=meta.at[k], dst_ref=got.at[source],
            send_sem=meta_send.at[k], recv_sem=meta_recv.at[source],
            device_id={"owners": a, "sub": b}, device_id_type=MESH,
        )

    def step(k, c):
        fill(k)
        row_copy(k - 1, own).start()
        return c

    fill(0)
    fill(1)
    pl.semaphore_wait(barrier, shards - 1)
    row_copy(0, own).start()
    lax.fori_loop(2, early, step, 0)

    square = emb[...].astype(f32)
    square = square * square
    square_hi = square.astype(bf16)
    square_lo = (square - square_hi.astype(f32)).astype(bf16)
    ones = jnp.ones((8, width), bf16)
    total = lax.dot_general(ones, square_hi, CROSS, preferred_element_type=f32)
    total = total + lax.dot_general(ones, square_lo, CROSS, preferred_element_type=f32)
    inverse_row = lax.rsqrt(total[0:1] + 1e-06)
    table_copy.wait()
    given = jnp.zeros((1, rows), f32)
    others = jnp.full((1, rows), -1e30, f32)
    for lo in range(0, classes, 128):
        n = min(128, classes - lo)
        part = table[lo : lo + n, :]
        part_f = part.astype(f32)
        inverse_class = lax.rsqrt(jnp.sum(part_f * part_f, axis=1, keepdims=True) + 1e-06)
        scaled = lax.dot_general(part, emb[...], CROSS, preferred_element_type=f32) * inverse_class
        match = lax.broadcasted_iota(i32, (n, rows), 0) + lo == near
        given = given + jnp.sum(jnp.where(match, scaled, 0.0), axis=0, keepdims=True)
        others = jnp.maximum(others, jnp.max(jnp.where(match, -1e30, scaled), axis=0, keepdims=True))
    margin = (20.0 * (given * inverse_row - others * inverse_row)).astype(bf16).astype(f32)
    rank_hot = (lax.broadcasted_iota(i32, (spots.shape[1], rows), 0) == rank).astype(f32).astype(bf16)
    spots[...] = lax.dot_general((shard_hot * margin).astype(bf16), rank_hot, CROSS, preferred_element_type=f32)
    counts = lax.dot_general(jnp.ones((8, rows), bf16), shard_bf, CROSS, preferred_element_type=f32)[0:1]

    def fill_meta(k, c):
        a, b = place(owners, subs, k)
        meta[k, 0:1, :] = spots[pl.ds(a * subs + b, 1), :]
        meta[k, 1:2, :] = counts
        return c

    lax.fori_loop(0, shards - 1, fill_meta, 0)
    got[own, 0:1, :] = spots[pl.ds(own, 1), :]
    got[own, 1:2, :] = counts

    lax.fori_loop(early, early + 1, step, 0)

    def send_meta(k, c):
        meta_copy(k, own).start()
        return c

    lax.fori_loop(0, shards - 1, send_meta, 0)
    lax.fori_loop(early + 1, shards, step, 0)
    own_copy = pltpu.make_async_copy(send.at[shards - 1], rows_ref.at[own], own_sem)
    own_copy.start()

    def take_meta(k, c):
        source = (own + 1 + k) % shards
        meta_copy(k, source).wait_recv()
        return c

    lax.fori_loop(0, shards - 1, take_meta, 0)

    def lay(s, c):
        scores_s[pl.ds(s, 1), :] = got[s, 0:1, :]
        counts_s[pl.ds(s, 1), :] = got[s, 1:2, :]
        return c

    lax.fori_loop(0, shards, lay, 0)
    table_counts = counts_s[...]
    totals_ref[...] = jnp.sum(table_counts, axis=0, keepdims=True).astype(i32)
    below = (
        lax.broadcasted_iota(i32, (shards, shards), 1) < lax.broadcasted_iota(i32, (shards, shards), 0)
    ).astype(f32)
    before = jnp.dot(below, table_counts, preferred_element_type=f32, precision=lax.Precision.HIGHEST)
    mine = lax.broadcasted_iota(i32, (shards, wide), 1) == own
    count_col = jnp.sum(jnp.where(mine, table_counts, 0.0), axis=1, keepdims=True).astype(i32)
    before_col = jnp.sum(jnp.where(mine, before, 0.0), axis=1, keepdims=True).astype(i32)
    offset = lax.broadcasted_iota(i32, (shards, slots), 1) - cap * lax.broadcasted_iota(i32, (shards, slots), 0)
    inside = (offset >= 0) & (offset < cap)
    spot = jnp.sum(jnp.where(inside, offset, 0), axis=0, keepdims=True)
    filled = jnp.where(offset < count_col, before_col + offset, -1)
    position_ref[...] = jnp.sum(jnp.where(inside, filled, 0), axis=0, keepdims=True)
    spread = (lax.broadcasted_iota(i32, (wide, slots), 0) == spot).astype(f32).astype(bf16)
    flat = jnp.dot(scores_s[...].astype(bf16), spread, preferred_element_type=f32)
    score_ref[...] = jnp.sum(jnp.where(inside, flat, 0.0), axis=0, keepdims=True).astype(score_ref.dtype)

    def finish(k, c):
        source = (own + 1 + k) % shards
        row_copy(k, source).wait_recv()
        row_copy(k, own).wait_send()
        meta_copy(k, own).wait_send()
        return c

    lax.fori_loop(0, shards - 1, finish, 0)
    own_copy.wait()


def quick_kernel(groups, owners, subs, cap, base, depth, near_hbm, keep_hbm, dest_hbm, emb_hbm, table_hbm,
                 rows_ref, score_ref, position_ref, totals_ref, flag_ref,
                 near_ref, keep_ref, dest_ref, emb, table, keep2, earlier, send, spare, spill, news, heard, told, scored,
                 heard_s, scores_s, slot_s, verdict,
                 in_sem, send_sem, recv_sem, news_send, news_recv, score_send, score_recv, spare_send, spare_recv,
                 relay_send, relay_recv, flag_send, flag_recv, own_sem, mutual):
    f32, bf16, i32 = jnp.float32, jnp.bfloat16, jnp.int32
    shards = owners * subs
    rows, width = emb.shape
    classes = table.shape[0]
    wide = news.shape[2]
    lead = wide - shards
    slots = shards * cap
    g, o, z = lax.axis_index("groups"), lax.axis_index("owners"), lax.axis_index("sub")
    own = o * subs + z
    peers = [(o + 1 + i) % owners for i in range(owners)]
    planes = [place(owners, subs, j * owners)[1] for j in range(subs)]
    low = 1 - (2 * z) // subs
    planes = [b + low * ((2 * b) // subs) * (subs // 2 + subs - 1 - 2 * b) for b in planes]

    small = [
        pltpu.make_async_copy(near_hbm, near_ref, in_sem.at[2]),
        pltpu.make_async_copy(keep_hbm, keep_ref, in_sem.at[3]),
        pltpu.make_async_copy(dest_hbm, dest_ref, in_sem.at[4]),
    ]
    for copy in small:
        copy.start()
    emb_copy = pltpu.make_async_copy(emb_hbm, emb, in_sem.at[0])
    emb_copy.start()
    table_copy = pltpu.make_async_copy(table_hbm, table, in_sem.at[1])
    table_copy.start()

    def device(j, i):
        return {"owners": peers[i], "sub": planes[j]}

    pairs = [(j, i) for j in range(subs) for i in range(owners)][: shards - 1]
    half = subs // 2
    upper = (2 * z) // subs
    cross = [(1 - upper) * (subs - 1 - m) + upper * m for m in range(half)]
    mates = [upper * half + (z - upper * half + m) % half for m in range(1, half)]
    barrier = pltpu.get_barrier_semaphore()
    for b in cross:
        for a in peers:
            pl.semaphore_signal(barrier, inc=1, device_id={"owners": a, "sub": b}, device_id_type=MESH)
    for i in range(1, groups):
        pl.semaphore_signal(barrier, inc=1, device_id={"groups": (g + i) % groups}, device_id_type=MESH)

    earlier[...] = (
        lax.broadcasted_iota(i32, (rows, rows), 0) < lax.broadcasted_iota(i32, (rows, rows), 1)
    ).astype(f32).astype(bf16)
    keep2[...] = jnp.zeros_like(keep2)
    for copy in small:
        copy.wait()
    near = near_ref[...]
    target = dest_ref[...]
    for h in range(up(classes, 128) // 128):
        n = min(128, classes - h * 128)
        keep2[h : h + 1, :n] = keep_ref[:, h * 128 : h * 128 + n].astype(f32)
    deep = keep2.shape[0]
    high = near // 128
    low = near - high * 128
    low_hot = (lax.broadcasted_iota(i32, (128, rows), 0) == low).astype(f32).astype(bf16)
    by_high = jnp.dot(keep2[...].astype(bf16), low_hot, preferred_element_type=f32)
    kept = jnp.sum(
        jnp.where(lax.broadcasted_iota(i32, (deep, rows), 0) == high, by_high, 0.0), axis=0, keepdims=True
    )
    shard_hot = jnp.where(lax.broadcasted_iota(i32, (up(shards, 8), rows), 0) == target, kept, 0.0)
    running = jnp.dot(shard_hot.astype(bf16), earlier[...], preferred_element_type=f32)
    rank = jnp.sum(shard_hot * running, axis=0, keepdims=True).astype(i32)
    slot_s[...] = jnp.where(kept > 0.5, target * cap + rank, -1)

    ahead = target - target // subs * subs - z
    ahead = jnp.where(ahead < 0, ahead + subs, ahead)
    over = (kept > 0.5) & (rank >= base) & (ahead > 0)
    plane_hot = jnp.where((lax.broadcasted_iota(i32, (up(subs, 8), rows), 0) == ahead) & over, 1.0, 0.0)
    before_it = jnp.dot(plane_hot.astype(bf16), earlier[...], preferred_element_type=f32)
    spot = jnp.sum(plane_hot * before_it, axis=0, keepdims=True).astype(i32)
    fits = over & (spot < depth)
    nth = jnp.where(fits, spot + 1, 0).astype(f32)

    rank_hot = (lax.broadcasted_iota(i32, (wide, rows), 0) == rank).astype(f32).astype(bf16)
    count_hot = jnp.where(lax.broadcasted_iota(i32, (wide, rows), 0) == target + lead, kept, 0.0).astype(bf16)
    notes = lax.dot_general((shard_hot * nth).astype(bf16), rank_hot, CROSS, preferred_element_type=f32)
    notes = notes + lax.dot_general(
        jnp.ones((up(shards, 8), rows), bf16), count_hot, CROSS, preferred_element_type=f32
    )
    for t in range(shards):
        news[t] = notes[t : t + 1]
    heard[own] = news[own]

    emb_copy.wait()

    seat = jnp.where(fits, (ahead - 1) * depth + spot, -1)
    hot = (lax.broadcasted_iota(i32, ((subs - 1) * depth, rows), 0) == seat).astype(f32).astype(bf16)
    packed = jnp.dot(hot, emb[...], preferred_element_type=f32).astype(bf16)
    for d in range(subs - 1):
        spare[d] = packed[d * depth : (d + 1) * depth]

    def fill(j, n):
        slot = slot_s[...] - planes[j] * cap
        hot = jnp.concatenate([
            (slot - a * subs * cap == lax.broadcasted_iota(i32, (n, rows), 0)).astype(f32).astype(bf16) for a in peers
        ])
        block = jnp.dot(hot, emb[...], preferred_element_type=f32).astype(bf16)
        for i in range(owners):
            send[j * owners + i, :n] = block[i * n : (i + 1) * n]

    def row_copy(j, i, n):
        k = j * owners + i
        return pltpu.make_async_remote_copy(
            src_ref=send.at[k, :n], dst_ref=rows_ref.at[own, :n],
            send_sem=send_sem.at[k], recv_sem=recv_sem.at[own],
            device_id=device(j, i), device_id_type=MESH,
        )

    def row_arrival(j, i, n):
        source = peers[i] * subs + planes[j]
        return pltpu.make_async_remote_copy(
            src_ref=send.at[0, :n], dst_ref=rows_ref.at[source, :n],
            send_sem=send_sem.at[0], recv_sem=recv_sem.at[source],
            device_id=device(j, i), device_id_type=MESH,
        )

    def note_copy(a, b, ref, landing, out_sem, in_sem, source):
        t = a * subs + b
        return pltpu.make_async_remote_copy(
            src_ref=ref.at[t], dst_ref=landing.at[source],
            send_sem=out_sem.at[t], recv_sem=in_sem.at[source],
            device_id={"owners": a, "sub": b}, device_id_type=MESH,
        )

    def news_copy(a, b, source):
        return note_copy(a, b, news, heard, news_send, news_recv, source)

    def score_copy(j, i, source):
        return note_copy(peers[i], planes[j], told, scored, score_send, score_recv, source)

    ways = [(b - z + subs) % subs for b in planes[: subs - 1]]

    def spare_copy(b, arrival=False):
        way = (b - z + subs) % subs
        slot = way - 1 if arrival else subs - 1 - way
        return pltpu.make_async_remote_copy(
            src_ref=spare.at[way - 1], dst_ref=spill.at[o, slot],
            send_sem=spare_send.at[way - 1], recv_sem=spare_recv.at[slot],
            device_id={"owners": o, "sub": b}, device_id_type=MESH,
        )

    def relay_copy(i, j, source):
        slot = ways[j] - 1
        return pltpu.make_async_remote_copy(
            src_ref=spill.at[source, slot], dst_ref=spill.at[source, slot],
            send_sem=relay_send.at[i, slot], recv_sem=relay_recv.at[source, slot],
            device_id={"owners": peers[i], "sub": z}, device_id_type=MESH,
        )

    def flag_copy(i, source):
        return pltpu.make_async_remote_copy(
            src_ref=verdict.at[g], dst_ref=verdict.at[source],
            send_sem=flag_send.at[i], recv_sem=flag_recv.at[source],
            device_id={"groups": (g + i) % groups}, device_id_type=MESH,
        )

    pl.semaphore_wait(barrier, half * owners + groups - 1)
    pl.semaphore_signal(
        mutual, inc=1, device_id={"owners": o, "sub": (z + half) % subs}, device_id_type=MESH
    )
    for b in cross:
        spare_copy(b).start()
    for b in cross:
        for a in peers:
            news_copy(a, b, own).start()
    fill(0, base)
    for i in range(owners):
        row_copy(0, i, base).start()
    fill(subs - 1, cap)
    pl.semaphore_wait(mutual, 1)
    for b in mates:
        spare_copy(b).start()
    for b in [*mates, z]:
        for a in peers[: owners - 1] if b is z else peers:
            news_copy(a, b, own).start()
    for i in range(owners - 1):
        row_copy(subs - 1, i, cap).start()
    own_copy = pltpu.make_async_copy(send.at[shards - 1], rows_ref.at[own], own_sem)
    own_copy.start()
    square = emb[...].astype(f32)
    square = square * square
    square_hi = square.astype(bf16)
    square_lo = (square - square_hi.astype(f32)).astype(bf16)
    ones = jnp.ones((8, width), bf16)
    total = lax.dot_general(ones, square_hi, CROSS, preferred_element_type=f32)
    total = total + lax.dot_general(ones, square_lo, CROSS, preferred_element_type=f32)
    inverse_row = lax.rsqrt(total[0:1] + 1e-06)
    table_copy.wait()
    given = jnp.zeros((1, rows), f32)
    others = jnp.full((1, rows), -1e30, f32)
    for lo in range(0, classes, 128):
        n = min(128, classes - lo)
        part = table[lo : lo + n, :]
        part_f = part.astype(f32)
        inverse_class = lax.rsqrt(jnp.sum(part_f * part_f, axis=1, keepdims=True) + 1e-06)
        scaled = lax.dot_general(part, emb[...], CROSS, preferred_element_type=f32) * inverse_class
        match = lax.broadcasted_iota(i32, (n, rows), 0) + lo == near
        given = given + jnp.sum(jnp.where(match, scaled, 0.0), axis=0, keepdims=True)
        others = jnp.maximum(others, jnp.max(jnp.where(match, -1e30, scaled), axis=0, keepdims=True))
    margin = (20.0 * (given * inverse_row - others * inverse_row)).astype(bf16).astype(f32)
    rank_hot = (lax.broadcasted_iota(i32, (wide, rows), 0) == rank).astype(f32).astype(bf16)
    marks = lax.dot_general((shard_hot * margin).astype(bf16), rank_hot, CROSS, preferred_element_type=f32)
    for t in range(shards):
        told[t] = marks[t : t + 1]
    scored[own] = told[own]
    fill(1, base)
    for j, i in pairs:
        score_copy(j, i, own).start()
    for j in range(1, subs - 1):
        if j > 1:
            fill(j, base)
        for i in range(owners):
            row_copy(j, i, base).start()
    order = [*range(1, subs - 1), 0]
    for j in order:
        spare_copy(planes[j], True).wait_recv()
        for i in range(owners - 1):
            relay_copy(i, j, o).start()

    for j, i in pairs:
        news_copy(peers[i], planes[j], peers[i] * subs + planes[j]).wait_recv()
    for t in range(shards):
        heard_s[t : t + 1, :] = heard[t]
    counts = jnp.where(lax.broadcasted_iota(i32, (shards, wide), 1) >= lead, heard_s[...], 0.0)
    row_i, col_i = lax.broadcasted_iota(i32, (wide, wide), 0), lax.broadcasted_iota(i32, (wide, wide), 1)
    plane = ((row_i >= lead) & ((row_i - lead) % subs == col_i)).astype(f32)
    past = jnp.dot(jnp.maximum(counts - base, 0.0), plane, preferred_element_type=f32)
    away = lax.broadcasted_iota(i32, (shards, wide), 0) % subs != lax.broadcasted_iota(i32, (shards, wide), 1)
    most = jnp.max(jnp.max(jnp.where(away, past, 0.0), axis=1, keepdims=True), axis=0, keepdims=True)
    verdict[g] = jnp.broadcast_to(most, (1, wide))

    totals_ref[...] = jnp.sum(counts, axis=0, keepdims=True)[:, lead:].astype(i32)
    below = (
        lax.broadcasted_iota(i32, (shards, shards), 1) < lax.broadcasted_iota(i32, (shards, shards), 0)
    ).astype(f32)
    before = jnp.dot(below, counts, preferred_element_type=f32, precision=lax.Precision.HIGHEST)
    mine = lax.broadcasted_iota(i32, (shards, wide), 1) == own + lead
    count_col = jnp.sum(jnp.where(mine, counts, 0.0), axis=1, keepdims=True).astype(i32)
    before_col = jnp.sum(jnp.where(mine, before, 0.0), axis=1, keepdims=True).astype(i32)
    for i in range(1, groups):
        flag_copy(i, g).start()
    offset = lax.broadcasted_iota(i32, (shards, slots), 1) - cap * lax.broadcasted_iota(i32, (shards, slots), 0)
    inside = (offset >= 0) & (offset < cap)
    nook = jnp.sum(jnp.where(inside, offset, 0), axis=0, keepdims=True)
    filled = jnp.where(offset < count_col, before_col + offset, -1)
    position_ref[...] = jnp.sum(jnp.where(inside, filled, 0), axis=0, keepdims=True)

    def merge(a, j):
        s = a * subs + planes[j]
        nth_row = heard[s][:, base:cap].astype(i32)
        pick = (lax.broadcasted_iota(i32, (depth, cap - base), 0) + 1 == nth_row).astype(f32).astype(bf16)
        rest = lax.dot_general(pick, spill[a, ways[j] - 1], DOWN, preferred_element_type=f32)
        rows_ref[s, base:cap] = rest.astype(bf16)

    for j in order:
        merge(o, j)
    for i in range(1, groups):
        flag_copy(i, (g + groups - i) % groups).wait_recv()
    flag_ref[0] = (jnp.max(verdict[...]) > depth).astype(i32)
    for j in order:
        for i in range(owners - 1):
            relay_copy(i, j, peers[i]).wait_recv()
            merge(peers[i], j)

    for j, i in pairs:
        score_copy(j, i, peers[i] * subs + planes[j]).wait_recv()
    for t in range(shards):
        scores_s[t : t + 1, :] = scored[t]
    spread = (lax.broadcasted_iota(i32, (wide, slots), 0) == nook).astype(f32).astype(bf16)
    flat = jnp.dot(scores_s[...].astype(bf16), spread, preferred_element_type=f32)
    score_ref[...] = jnp.sum(jnp.where(inside, flat, 0.0), axis=0, keepdims=True).astype(score_ref.dtype)

    for i in range(1, groups):
        flag_copy(i, g).wait_send()
    for j in range(subs - 1):
        spare_copy(planes[j]).wait_send()
    for j in range(subs - 1):
        for i in range(owners - 1):
            relay_copy(i, j, o).wait_send()
    own_copy.wait()
    for j, i in pairs:
        news_copy(peers[i], planes[j], own).wait_send()
        score_copy(j, i, own).wait_send()
        row_copy(j, i, base if j < subs - 1 else cap).wait_send()
    for j, i in pairs:
        row_arrival(j, i, base if j < subs - 1 else cap).wait_recv()


def plain(call, embeddings, class_table, nearest, keep_class, destination):
    owners, subs = lax.axis_size("owners"), lax.axis_size("sub")
    shards = owners * subs
    rows, width = embeddings.shape
    classes = class_table.shape[0]
    cap = 3 * rows // (2 * shards)
    wide = up(max(shards, cap), 128)
    early = max(2, shards // 4)
    vmem = pl.BlockSpec(memory_space=pltpu.VMEM)
    hbm = pl.BlockSpec(memory_space=pl.ANY)
    f32, bf16, i32 = jnp.float32, jnp.bfloat16, jnp.int32
    dma = pltpu.SemaphoreType.DMA
    return pl.pallas_call(
        functools.partial(kernel, owners, subs, cap, early),
        out_shape=(
            pltpu.VMEM((shards, cap, width), bf16),
            pltpu.VMEM((1, shards * cap), f32),
            pltpu.VMEM((1, shards * cap), i32),
            pltpu.VMEM((1, wide), i32),
        ),
        in_specs=[hbm] * 5,
        out_specs=(vmem,) * 4,
        scratch_shapes=[
            pltpu.VMEM((1, rows), i32),
            pltpu.VMEM((1, classes), i32),
            pltpu.VMEM((1, rows), i32),
            pltpu.VMEM((rows, width), bf16),
            pltpu.VMEM((classes, width), bf16),
            pltpu.VMEM((up(up(classes, 128) // 128, 8), 128), f32),
            pltpu.VMEM((shards, cap, width), bf16),
            pltpu.VMEM((shards, 2, wide), f32),
            pltpu.VMEM((shards, 2, wide), f32),
            pltpu.VMEM((wide, wide), f32),
            pltpu.VMEM((shards, wide), f32),
            pltpu.VMEM((shards, wide), f32),
            pltpu.VMEM((1, rows), i32),
            dma((5,)),
            dma((shards,)),
            dma((shards,)),
            dma((shards,)),
            dma((shards,)),
            dma,
        ],
        compiler_params=pltpu.CompilerParams(collective_id=call, has_side_effects=True),
    )(
        nearest.reshape(1, rows),
        keep_class.reshape(1, classes),
        destination.reshape(1, rows),
        embeddings,
        class_table,
    )


def quick(base, depth, embeddings, class_table, nearest, keep_class, destination):
    groups, owners, subs = lax.axis_size("groups"), lax.axis_size("owners"), lax.axis_size("sub")
    shards = owners * subs
    rows, width = embeddings.shape
    classes = class_table.shape[0]
    cap = 3 * rows // (2 * shards)
    wide = up(shards + cap, 128)
    vmem = pl.BlockSpec(memory_space=pltpu.VMEM)
    hbm = pl.BlockSpec(memory_space=pl.ANY)
    f32, bf16, i32 = jnp.float32, jnp.bfloat16, jnp.int32
    dma = pltpu.SemaphoreType.DMA
    return pl.pallas_call(
        functools.partial(quick_kernel, groups, owners, subs, cap, base, depth),
        out_shape=(
            pltpu.VMEM((shards, cap, width), bf16),
            pltpu.VMEM((1, shards * cap), f32),
            pltpu.VMEM((1, shards * cap), i32),
            pltpu.VMEM((1, shards), i32),
            pltpu.SMEM((1,), i32),
        ),
        in_specs=[hbm] * 5,
        out_specs=(vmem,) * 4 + (pl.BlockSpec(memory_space=pltpu.SMEM),),
        scratch_shapes=[
            pltpu.VMEM((1, rows), i32),
            pltpu.VMEM((1, classes), i32),
            pltpu.VMEM((1, rows), i32),
            pltpu.VMEM((rows, width), bf16),
            pltpu.VMEM((classes, width), bf16),
            pltpu.VMEM((up(up(classes, 128) // 128, 8), 128), f32),
            pltpu.VMEM((rows, rows), bf16),
            pltpu.VMEM((shards, cap, width), bf16),
            pltpu.VMEM((subs - 1, depth, width), bf16),
            pltpu.VMEM((owners, subs - 1, depth, width), bf16),
            pltpu.VMEM((shards, 1, wide), f32),
            pltpu.VMEM((shards, 1, wide), f32),
            pltpu.VMEM((shards, 1, wide), f32),
            pltpu.VMEM((shards, 1, wide), f32),
            pltpu.VMEM((shards, wide), f32),
            pltpu.VMEM((shards, wide), f32),
            pltpu.VMEM((1, rows), i32),
            pltpu.VMEM((groups, 1, wide), f32),
            dma((5,)),
            dma((shards,)),
            dma((shards,)),
            dma((shards,)),
            dma((shards,)),
            dma((shards,)),
            dma((shards,)),
            dma((subs - 1,)),
            dma((subs - 1,)),
            dma((owners, subs - 1)),
            dma((owners, subs - 1)),
            dma((groups,)),
            dma((groups,)),
            dma,
            pltpu.SemaphoreType.REGULAR,
        ],
        compiler_params=pltpu.CompilerParams(collective_id=0, has_side_effects=True),
    )(
        nearest.reshape(1, rows),
        keep_class.reshape(1, classes),
        destination.reshape(1, rows),
        embeddings,
        class_table,
    )


def close(got_rows, score, position, totals):
    shards, cap, width = got_rows.shape
    wide = totals.shape[1]
    vmem = pl.BlockSpec(memory_space=pltpu.VMEM)
    hbm = pl.BlockSpec(memory_space=pl.ANY)
    bf16, i32 = jnp.bfloat16, jnp.int32
    dma = pltpu.SemaphoreType.DMA
    small = [pltpu.with_memory_space_constraint(x, pltpu.VMEM) for x in (got_rows, score, position, totals)]
    rows_out, score_out, position_out, totals_out = pl.pallas_call(
        finish_kernel,
        out_shape=(
            jax.ShapeDtypeStruct((shards, cap, width), bf16),
            jax.ShapeDtypeStruct((shards * cap,), bf16),
            jax.ShapeDtypeStruct((shards * cap,), i32),
            jax.ShapeDtypeStruct((wide,), i32),
        ),
        in_specs=[vmem] * 4,
        out_specs=(hbm,) * 4,
        scratch_shapes=[
            pltpu.VMEM((shards * cap,), bf16),
            pltpu.VMEM((shards * cap,), i32),
            pltpu.VMEM((wide,), i32),
            dma((4,)),
        ],
    )(*small)
    return rows_out.reshape(shards * cap, width), score_out, position_out, totals_out[:shards]


def on_device(*args):
    rows = args[0].shape[0]
    subs, shards = lax.axis_size("sub"), lax.axis_size("owners") * lax.axis_size("sub")
    cap = 3 * rows // (2 * shards)
    base, depth = 2 * cap // 3, cap // 2
    if subs % 2 or shards % 8 or base % 16 or cap % 16 or depth % 8:
        return close(*plain(0, *args))
    *packed, flag = quick(base, depth, *args)

    def fast(inputs, results):
        return close(*results)

    def slow(inputs, results):
        return close(*plain(1, *inputs))

    return lax.cond(flag.reshape(()) > 0, slow, fast, args, tuple(packed))


def solution(mesh):
    in_specs = (
        P(("groups", "owners", "sub"), None),
        P(),
        P(("groups", "owners", "sub")),
        P(),
        P(("groups", "owners", "sub"), None),
    )
    out_specs = (
        P(("groups", "owners", "sub"), None),
        P(("groups", "owners", "sub")),
        P(("groups", "owners", "sub")),
        P("groups"),
    )
    return jax.shard_map(
        on_device, mesh=mesh, in_specs=in_specs, out_specs=out_specs, check_vma=False
    )
```
